32 devices in a mesh: sx: 4 (over y, x), sy: 8 (over z, core).
Axes of the slice: x: 2, y: 2, z: 4, core: 2. Of those that a mesh axis runs over, the one named last changes fastest.
Arguments:
- forward_weights: float32 [4096, 8, 432], P(('sy', 'sx')), may hold values from -6 to 6
- adjoint_weights: float32 [32768, 432], P(('sx', 'sy')), may hold values from -6 to 6
- medium: float32 [4], replicated, may hold values from 0.2 to 0.6
Outputs:
- forward_out: float32 [32768, 432], P(('sx', 'sy'))
- adjoint_out: float32 [8, 4096, 432], P(None, ('sy', 'sx'))
The draws below stay inside these ranges and needn't reach their ends.
All inputs are finite; a program needn't handle non-finite values.
Results may differ from the reference program's by a relative error of at most 0.0003.
Values sent between devices are 32-bit elements; how exact they have to be, the bound alone decides.
A program may use at most 128 MiB of HBM per device.

```python
import math
import jax
import jax.numpy as jnp
import numpy as np
from jax import lax

ORDER = 6
LEVELS = 4
TGT0 = 8
SHOTS = 1
Q = 216
SRC = 4096
TGT = 32768


def shard_levels(own_key, extent, cuts, smallest, top_value):
    level, own = 1.0, jax.random.fold_in(own_key, 6)
    for position, parts in cuts:
        heights = jnp.exp(jax.random.uniform(jax.random.fold_in(own, position), (parts,), jnp.float32, smallest / len(cuts), top_value / len(cuts)))
        level = level * jnp.repeat(heights, extent[position] // parts).reshape([-1 if axis == position else 1 for axis in range(len(extent))])
    return level


def scatter_about(key, extent, scale, bound, cuts=(), held_as=jnp.bfloat16):
    gain = shard_levels(key, extent, cuts, -0.22, 0.18) if cuts else 1.0
    entries = jax.random.normal(key, extent, jnp.float32) * scale * gain
    return jnp.minimum(jnp.maximum(entries, -bound), bound).astype(held_as)


def setup_inputs(seed: int = 0) -> dict:
    seeds = jax.random.split(jax.random.key(seed), 4)
    forward_weights = scatter_about(seeds[0], (SRC, TGT0, 2 * SHOTS * Q), 1.0, 6.0, ((0, 32),), jnp.float32)
    adjoint_weights = scatter_about(seeds[1], (TGT, 2 * SHOTS * Q), 1.0, 6.0, ((0, 32),), jnp.float32)
    medium = jnp.clip(jax.random.uniform(seeds[2], (4,), jnp.float32, 0.2, 0.6), 0.2, 0.6)
    return {"forward_weights": forward_weights, "adjoint_weights": adjoint_weights, "medium": medium}


two_pi = 2.0 * math.pi
shrink = 1.0 / math.sqrt(8.0)
band = 8.0

def cheb_points(order_count):
    return np.array([(1.0 - math.cos((2 * node_index + 1) * math.pi / (2 * order_count))) / 2.0 for node_index in range(order_count)])

def child_table(order_count):
    nodes_here = cheb_points(order_count)
    halves = []
    for offset_bit in range(2):
        matrix = np.zeros((order_count, order_count))
        for row_index in range(order_count):
            where_at = (nodes_here[row_index] + offset_bit) / 2.0
            for col_index in range(order_count):
                value_now = 1.0
                for other_index in range(order_count):
                    if other_index != col_index:
                        value_now *= (where_at - nodes_here[other_index]) / (nodes_here[col_index] - nodes_here[other_index])
                matrix[row_index, col_index] = value_now
        halves.append(matrix)
    blocks_out = []
    for child_index in range(8):
        along_x = halves[child_index // 4]
        along_y = halves[child_index // 2 % 2]
        along_z = halves[child_index % 2]
        blocks_out.append(np.kron(np.kron(along_x, along_y), along_z))
    return jnp.asarray(np.stack(blocks_out), dtype=jnp.float32)

def box_digits(box_index, groups):
    coord_x = jnp.zeros_like(box_index)
    coord_y = jnp.zeros_like(box_index)
    coord_z = jnp.zeros_like(box_index)
    for group_now in range(groups):
        digit_now = box_index // 8 ** (groups - 1 - group_now) % 8
        coord_x = coord_x * 2 + digit_now // 4
        coord_y = coord_y * 2 + digit_now // 2 % 2
        coord_z = coord_z * 2 + digit_now % 2
    return jnp.stack([coord_x, coord_y, coord_z], axis=-1).astype(jnp.float32)

def box_centres(box_index, groups):
    return (box_digits(box_index, groups) + 0.5) / float(2 ** groups)

def box_points(box_index, groups):
    box_side = band / float(2 ** groups)
    nodes_here = jnp.asarray(cheb_points(ORDER), dtype=jnp.float32)
    grid_x = jnp.repeat(nodes_here, ORDER * ORDER)
    grid_y = jnp.tile(jnp.repeat(nodes_here, ORDER), ORDER)
    grid_z = jnp.tile(nodes_here, ORDER * ORDER)
    offsets = jnp.stack([grid_x, grid_y, grid_z], axis=-1)
    corner = box_digits(box_index, groups)
    return box_side * (corner[..., None, :] + offsets)

def phase_angle(centres, points, medium):
    along = lax.optimization_barrier(jnp.sum(centres * points, axis=-1))
    radius = jnp.sqrt(lax.optimization_barrier(jnp.sum(points * points, axis=-1)))
    travel = medium[0] + lax.optimization_barrier(jnp.sum(medium[1:] * centres, axis=-1))
    return two_pi * (along + travel * radius)

def complex_turn(real_part, imag_part, angle_now, sign_now):
    cosine = jnp.cos(angle_now)
    sine_part = sign_now * jnp.sin(angle_now)
    return (real_part * cosine - imag_part * sine_part, real_part * sine_part + imag_part * cosine)

def forward_level(weights, src_off, tgt_off, level_now, medium, interp):
    src_count, tgt_count = (weights.shape[0], weights.shape[1])
    shot_count, point_count = (weights.shape[3], weights.shape[4])
    parent_count = src_count // 8
    new_targets = tgt_off * 8 + jnp.arange(tgt_count * 8, dtype=jnp.int32)
    centres = box_centres(new_targets, level_now + 2).reshape(tgt_count, 8, 3)
    children = src_off + jnp.arange(src_count, dtype=jnp.int32)
    child_points = box_points(children, LEVELS - level_now).reshape(parent_count, 8, point_count, 3)
    parents = src_off // 8 + jnp.arange(parent_count, dtype=jnp.int32)
    parent_points = box_points(parents, LEVELS - level_now - 1)
    theta_in = phase_angle(centres[None, None, :, :, None, :], child_points[:, :, None, None, :, :], medium)
    theta_out = phase_angle(centres[None, :, :, None, :], parent_points[:, None, None, :, :], medium)
    shaped = weights.reshape(parent_count, 8, tgt_count, 1, 2, shot_count, point_count)
    turned = complex_turn(shaped[:, :, :, :, 0], shaped[:, :, :, :, 1], theta_in[:, :, :, :, None, :], 1.0)
    stacked = jnp.stack(turned, axis=4)
    mixed = jnp.einsum('pctkxhq,cqs->ptkxhs', stacked, interp, precision=lax.Precision.HIGHEST)
    result_re, result_im = complex_turn(mixed[:, :, :, 0], mixed[:, :, :, 1], theta_out[:, :, :, None, :], -1.0)
    output = shrink * jnp.stack([result_re, result_im], axis=3)
    return output.reshape(parent_count, tgt_count * 8, 2, shot_count, point_count)

def adjoint_level(values, tgt_off, src_off, level_now, medium, interp):
    tgt_count, src_count = (values.shape[0], values.shape[1])
    shot_count, point_count = (values.shape[3], values.shape[4])
    parent_count = tgt_count // 8
    targets = tgt_off + jnp.arange(tgt_count, dtype=jnp.int32)
    centres = box_centres(targets, level_now + 2).reshape(parent_count, 8, 3)
    sources = src_off + jnp.arange(src_count, dtype=jnp.int32)
    source_points = box_points(sources, LEVELS - level_now - 1)
    children = src_off * 8 + jnp.arange(src_count * 8, dtype=jnp.int32)
    child_points = box_points(children, LEVELS - level_now).reshape(src_count, 8, point_count, 3)
    theta_out = phase_angle(centres[:, :, None, None, :], source_points[None, None, :, :, :], medium)
    theta_in = phase_angle(centres[:, :, None, None, None, :], child_points[None, None, :, :, :, :], medium)
    shaped = values.reshape(parent_count, 8, src_count, 2, shot_count, point_count)
    turned = complex_turn(shaped[:, :, :, 0], shaped[:, :, :, 1], theta_out[:, :, :, None, :], 1.0)
    stacked = jnp.stack(turned, axis=3)
    spread = jnp.einsum('pkbxhs,cqs->pkbcxhq', stacked, interp, precision=lax.Precision.HIGHEST)
    back_re, back_im = complex_turn(spread[:, :, :, :, 0], spread[:, :, :, :, 1], theta_in[:, :, :, :, None, :], -1.0)
    output = shrink * jnp.stack([lax.optimization_barrier(jnp.sum(back_re, axis=1)), lax.optimization_barrier(jnp.sum(back_im, axis=1))], axis=3)
    return output.reshape(parent_count, src_count * 8, 2, shot_count, point_count)

def blocked(level_fn, array_in):
    first_size, second_size = (array_in.shape[0], array_in.shape[1])
    block_ids = jnp.arange(8, dtype=jnp.int32)
    if first_size >= second_size:
        pieces = array_in.reshape((8, first_size // 8) + array_in.shape[1:])
        results = lax.map(lambda packed: level_fn(packed[0], packed[1] * (first_size // 8), jnp.int32(0)), (pieces, block_ids))
        return results.reshape((results.shape[0] * results.shape[1],) + results.shape[2:])
    pieces = jnp.swapaxes(array_in.reshape((first_size, 8, second_size // 8) + array_in.shape[2:]), 0, 1)
    results = lax.map(lambda packed: level_fn(packed[0], jnp.int32(0), packed[1] * (second_size // 8)), (pieces, block_ids))
    results = jnp.swapaxes(results, 0, 1)
    return results.reshape((results.shape[0], results.shape[1] * results.shape[2]) + results.shape[3:])

def reference(forward_weights, adjoint_weights, medium):
    interp = child_table(ORDER)
    current = forward_weights.reshape(forward_weights.shape[0], forward_weights.shape[1], 2, -1, Q)
    for level_now in range(LEVELS):
        current = blocked(lambda block_now, first_off, second_off: forward_level(block_now, first_off, second_off, level_now, medium, interp), current)
    forward_out = current.reshape(current.shape[1], -1)
    current = adjoint_weights.reshape(adjoint_weights.shape[0], 1, 2, -1, Q)
    for level_now in reversed(range(LEVELS)):
        current = blocked(lambda block_now, first_off, second_off: adjoint_level(block_now, first_off, second_off, level_now, medium, interp), current)
    adjoint_out = current.reshape(current.shape[0], current.shape[1], -1)
    return (forward_out, adjoint_out)
```

```python
import math

import jax
import jax.numpy as jnp
import ml_dtypes
import numpy as np
from jax import lax
from jax.experimental import pallas as pl
from jax.experimental.pallas import tpu as pltpu
from jax.sharding import PartitionSpec as P

ORDER = 6
LEVELS = 4
Q = 216
band = 8.0


def cheb_points(n):
    return np.array([(1.0 - math.cos((2 * i + 1) * math.pi / (2 * n))) / 2.0 for i in range(n)])


def child_table(n):
    g = cheb_points(n)
    halves = []
    for bit in range(2):
        m = np.ones((n, n))
        for r in range(n):
            w = (g[r] + bit) / 2.0
            for c in range(n):
                for o in range(n):
                    if o != c:
                        m[r, c] *= (w - g[o]) / (g[c] - g[o])
        halves.append(m)
    return np.stack(
        [np.kron(np.kron(halves[e // 4], halves[e // 2 % 2]), halves[e % 2]) for e in range(8)]
    )


def split_table(table):
    high = table.astype(ml_dtypes.bfloat16)
    low = (table - high.astype(np.float64)).astype(ml_dtypes.bfloat16)
    return jnp.asarray(high), jnp.asarray(low)


def box_coords(index, groups):
    coords = [jnp.zeros_like(index) for _ in range(3)]
    for group in range(groups):
        digit = index // 8 ** (groups - 1 - group) % 8
        bits = (digit // 4, digit // 2 % 2, digit % 2)
        coords = [c * 2 + b for c, b in zip(coords, bits)]
    return [c.astype(jnp.float32) for c in coords]


def point_slopes(src_off, count, groups, medium):
    side = band / float(2**groups)
    g = cheb_points(ORDER).astype(np.float32)
    grid = (np.repeat(g, ORDER * ORDER), np.tile(np.repeat(g, ORDER), ORDER), np.tile(g, ORDER**2))
    corner = box_coords(src_off + jnp.arange(count, dtype=jnp.int32), groups)
    pts = [side * (c[:, None] + o[None, :]) for c, o in zip(corner, grid)]
    radius = jnp.sqrt(pts[0] * pts[0] + pts[1] * pts[1] + pts[2] * pts[2])
    return [p + medium[d + 1] * radius for d, p in enumerate(pts)], medium[0] * radius


def turn_of(u):
    half = jnp.round(2.0 * u)
    y = (2.0 * math.pi) * (u - 0.5 * half)
    sign = 1.0 - 2.0 * (half - 2.0 * jnp.floor(0.5 * half))
    z = y * y
    s = jnp.float32(-1.0 / math.factorial(11))
    for n in (9, 7, 5, 3, 1):
        s = s * z + (1.0 if n % 4 == 1 else -1.0) / math.factorial(n)
    c = jnp.float32(1.0 / math.factorial(12))
    for n in (10, 8, 6, 4, 2, 0):
        c = c * z + (1.0 if n % 4 == 0 else -1.0) / math.factorial(n)
    return sign * c, sign * (s * y)


def pair_phase(src_off, src_count, src_groups, tgt_off, tgt_count, tgt_groups, medium):
    slopes, base = point_slopes(src_off, src_count, src_groups, medium)
    coords = box_coords(tgt_off + jnp.arange(tgt_count, dtype=jnp.int32), tgt_groups)
    u = base[:, None, :]
    for c, a in zip(coords, slopes):
        u = u + ((c + 0.5) / float(2**tgt_groups))[None, :, None] * a[:, None, :]
    return turn_of(u)


def child_phase(src_off, src_count, level, medium):
    slopes, _ = point_slopes(src_off, src_count, LEVELS - level, medium)
    k = np.arange(8)
    u = 0.0
    for bits, a in zip((k // 4, k // 2 % 2, k % 2), slopes):
        step = ((bits - 0.5) / 2.0 ** (level + 2)).astype(np.float32)
        u = u + step[None, :, None] * a[:, None, :]
    return jnp.stack(turn_of(u), axis=1)


def dot3(x, high, low):
    x_high = x.astype(jnp.bfloat16)
    x_low = (x - x_high.astype(jnp.float32)).astype(jnp.bfloat16)
    dot = lambda a, b: jnp.dot(a, b, preferred_element_type=jnp.float32)
    return dot(x_high, high) + dot(x_high, low) + dot(x_low, high)


def forward_kernel(x_ref, w_ref, high_ref, low_ref, o_ref):
    pb, _, _, tb, q = o_ref.shape[0], 2, 8, o_ref.shape[3], o_ref.shape[4]

    def step(e, acc):
        parts = []
        for p in range(pb):
            re, im = x_ref[p, e, 0], x_ref[p, e, 1]
            w_re, w_im = w_ref[p, e, 0], w_ref[p, e, 1]
            res = [re * w_re[k : k + 1] - im * w_im[k : k + 1] for k in range(8)]
            ims = [re * w_im[k : k + 1] + im * w_re[k : k + 1] for k in range(8)]
            parts += res + ims
        return acc + dot3(jnp.concatenate(parts, axis=0), high_ref[e], low_ref[e])

    acc = lax.fori_loop(0, 8, step, jnp.zeros((pb * 16 * tb, q), jnp.float32))
    o_ref[...] = acc.reshape(o_ref.shape)


def adjoint_kernel(y_ref, w_ref, high_ref, low_ref, o_ref):
    sb, tb, q = y_ref.shape[0], y_ref.shape[3], y_ref.shape[4]
    rows = y_ref[...].reshape(sb * 16 * tb, q)

    def step(e, carry):
        z = dot3(rows, high_ref[e], low_ref[e]).reshape(sb, 2, 8, tb, q)
        for s in range(sb):
            w_re, w_im = w_ref[s, e, 0], w_ref[s, e, 1]
            out_re = jnp.zeros((tb, q), jnp.float32)
            out_im = jnp.zeros((tb, q), jnp.float32)
            for k in range(8):
                re, im = z[s, 0, k], z[s, 1, k]
                c, d = w_re[k : k + 1], w_im[k : k + 1]
                out_re += re * c + im * d
                out_im += im * c - re * d
            o_ref[s, e, 0] = out_re
            o_ref[s, e, 1] = out_im
        return carry

    lax.fori_loop(0, 8, step, 0)


def blocks(count, tgt):
    tb = min(tgt, 32)
    return math.gcd(count, max(1, 32 // tb)), tb


def level_call(kernel, operand, phase, tables, out_shape):
    count, tgt, q = operand.shape[0], operand.shape[3], operand.shape[4]
    cb, tb = blocks(count, tgt)
    spec = lambda: pl.BlockSpec((cb, operand.shape[1], operand.shape[2], tb, q), lambda i, j: (i, 0, 0, j, 0))
    return pl.pallas_call(
        kernel,
        grid=(count // cb, tgt // tb),
        in_specs=[
            spec(),
            pl.BlockSpec((cb,) + phase.shape[1:], lambda i, j: (i, 0, 0, 0, 0)),
            pl.BlockSpec(tables[0].shape, lambda i, j: (0, 0, 0)),
            pl.BlockSpec(tables[1].shape, lambda i, j: (0, 0, 0)),
        ],
        out_specs=pl.BlockSpec((cb, out_shape[1], out_shape[2], tb, q), lambda i, j: (i, 0, 0, j, 0)),
        out_shape=jax.ShapeDtypeStruct(out_shape, jnp.float32),
        compiler_params=pltpu.CompilerParams(vmem_limit_bytes=56 * 1024 * 1024),
    )(operand, phase, *tables)


def general_forward_level(x, src_off, level, medium, tables):
    count, _, tgt, q = x.shape
    phase = child_phase(src_off, count, level, medium).reshape(count // 8, 8, 2, 8, q)
    out = level_call(
        forward_kernel, x.reshape(count // 8, 8, 2, tgt, q), phase, tables, (count // 8, 2, 8, tgt, q)
    )
    return out.swapaxes(2, 3).reshape(count // 8, 2, tgt * 8, q)


def general_adjoint_level(y, src_off, level, medium, tables):
    count, _, tgt, q = y.shape
    phase = child_phase(src_off * 8, count * 8, level, medium).reshape(count, 8, 2, 8, q)
    operand = y.reshape(count, 2, tgt // 8, 8, q).swapaxes(2, 3)
    out = level_call(adjoint_kernel, operand, phase, tables, (count, 8, 2, tgt // 8, q))
    return out.reshape(count * 8, 2, tgt // 8, q)


def general_shards(forward_weights, adjoint_weights, medium):
    table = child_table(ORDER) / math.sqrt(8.0)
    forward_tables = split_table(table)
    adjoint_tables = split_table(table.transpose(0, 2, 1))
    sizes = {a: lax.axis_size(a) for a in ("sx", "sy")}
    index = {a: lax.axis_index(a) for a in ("sx", "sy")}
    local_sources = forward_weights.shape[0]
    shots = forward_weights.shape[2] // (2 * Q)
    plan = []
    remaining = ["sx", "sy"]
    width = local_sources
    for _ in range(LEVELS):
        while width < 8:
            axis = remaining.pop(0)
            plan.append(axis)
            width *= sizes[axis]
        plan.append("level")
        width //= 8

    f_in = forward_weights.reshape(local_sources, -1, 2, shots, Q)
    b_in = adjoint_weights.reshape(adjoint_weights.shape[0], 2, shots, Q)
    f_src = (index["sy"] * sizes["sx"] + index["sx"]) * local_sources
    b_tgt = (index["sx"] * sizes["sy"] + index["sy"]) * adjoint_weights.shape[0]
    f_outs, b_outs = [], []
    for shot in range(shots):
        src, tgt, level = f_src, jnp.int32(0), 0
        re, im = f_in[:, :, 0, shot], f_in[:, :, 1, shot]
        c, s = pair_phase(src, re.shape[0], LEVELS, tgt, re.shape[1], 1, medium)
        x = jnp.stack([re * c - im * s, re * s + im * c], axis=1)
        for op in plan:
            if op == "level":
                x = general_forward_level(x, src, level, medium, forward_tables)
                src, tgt, level = src // 8, tgt * 8, level + 1
            else:
                n = sizes[op]
                count, _, width, _ = x.shape
                x = x.reshape(count, 2, n, width // n, Q).transpose(2, 0, 1, 3, 4)
                x = lax.all_to_all(x, op, split_axis=0, concat_axis=0, tiled=True)
                x = x.reshape(n * count, 2, width // n, Q)
                src = src - index[op] * count
                tgt = tgt + index[op] * (width // n)
        c, s = pair_phase(src, x.shape[0], LEVELS - level, tgt, x.shape[2], level + 1, medium)
        re, im = x[:, 0], x[:, 1]
        f_outs.append((re * c + im * s, im * c - re * s))
        src, tgt, level = jnp.int32(0), b_tgt, LEVELS
        re, im = b_in[None, :, 0, shot], b_in[None, :, 1, shot]
        c, s = pair_phase(src, 1, 0, tgt, re.shape[1], LEVELS + 1, medium)
        y = jnp.stack([re * c - im * s, re * s + im * c], axis=1)
        for op in reversed(plan):
            if op == "level":
                y = general_adjoint_level(y, src, level - 1, medium, adjoint_tables)
                src, tgt, level = src * 8, tgt // 8, level - 1
            else:
                n = sizes[op]
                count, _, width, _ = y.shape
                y = y.reshape(n, count // n, 2, width, Q)
                y = lax.all_to_all(y, op, split_axis=0, concat_axis=0, tiled=True)
                y = y.transpose(1, 2, 0, 3, 4).reshape(count // n, 2, n * width, Q)
                src = src + index[op] * (count // n)
                tgt = tgt - index[op] * width
        c, s = pair_phase(src, y.shape[0], LEVELS, tgt, y.shape[2], 1, medium)
        re, im = y[:, 0], y[:, 1]
        b_outs.append((re * c + im * s, im * c - re * s))
    f = jnp.stack([jnp.stack([o[i][0] for o in f_outs], axis=1) for i in range(2)], axis=1)
    b = jnp.stack([jnp.stack([o[i].swapaxes(0, 1) for o in b_outs], axis=2) for i in range(2)], axis=2)
    return f.reshape(f.shape[0], -1), b.reshape(b.shape[0], b.shape[1], -1)


HALF = Q // 2
ROWS = 512


def lane_points():
    t = np.arange(HALF)
    return t, (ORDER - 1 - t // ORDER**2) * ORDER**2 + t % ORDER**2


def parity_tables():
    t, m = lane_points()
    table = child_table(ORDER) / math.sqrt(8.0)
    out = np.zeros((4, 2, 256, 128))
    for e in range(4):
        rows = np.zeros((256, Q))
        rows[:HALF] = table[e][t]
        rows[128 : 128 + HALF] = table[e][m]
        for s, sign in enumerate((1.0, -1.0)):
            out[e, s, :, :HALF] = 0.5 * (rows[:, t] + sign * rows[:, m])
    high = out.astype(ml_dtypes.bfloat16)
    return high, (out - high.astype(np.float64)).astype(ml_dtypes.bfloat16)


def forward_parity_table():
    high, low = parity_tables()
    return jnp.asarray(np.concatenate([high, low], axis=-1))


def adjoint_parity_table():
    parts = [np.concatenate([x.swapaxes(-1, -2)] * 2, axis=2) for x in parity_tables()]
    return jnp.asarray(np.stack(parts, axis=2))


def grid_lanes():
    t, m = lane_points()
    g = cheb_points(ORDER).astype(np.float32)
    full = (np.repeat(g, ORDER * ORDER), np.tile(np.repeat(g, ORDER), ORDER), np.tile(g, ORDER**2))
    out = np.zeros((3, 256), np.float32)
    for d in range(3):
        out[d, :HALF], out[d, 128 : 128 + HALF] = full[d][t], full[d][m]
    return out


def lane_slopes(src_off, count, groups, medium):
    side = band / float(2**groups)
    grid = grid_lanes()
    corner = box_coords(src_off + jnp.arange(count, dtype=jnp.int32), groups)
    pts = [side * (c[:, None] + o[None, :]) for c, o in zip(corner, grid)]
    radius = jnp.sqrt(pts[0] * pts[0] + pts[1] * pts[1] + pts[2] * pts[2])
    return [p + medium[d + 1] * radius for d, p in enumerate(pts)], medium[0] * radius


def level_phase(src_off, count, level, medium):
    slopes, _ = lane_slopes(src_off, count, LEVELS - level, medium)
    k = np.arange(4)
    u = 0.0
    for bits, a in zip((k // 4, k // 2 % 2, k % 2), slopes):
        step = ((bits - 0.5) / 2.0 ** (level + 2)).astype(np.float32)
        u = u + step[None, :, None] * a[:, None, :]
    return jnp.concatenate(turn_of(u), axis=1)


def first_phase(src_off, count, medium):
    slopes, u = lane_slopes(src_off, count, LEVELS, medium)
    k = np.arange(8)
    u = u[:, None, :]
    for bits, a in zip((k // 4, k // 2 % 2, k % 2), slopes):
        u = u + ((bits + 0.5) / 2.0).astype(np.float32)[None, :, None] * a[:, None, :]
    return jnp.stack(turn_of(u), axis=1)


def last_phase(tgt_off, count, medium):
    slopes, base = lane_slopes(jnp.int32(0), 1, 0, medium)
    coords = box_coords(tgt_off // 64 + jnp.arange(count // 64, dtype=jnp.int32), LEVELS - 1)
    u = base
    for c, a in zip(coords, slopes):
        u = u + ((c + 0.5) / 2.0 ** (LEVELS - 1))[:, None] * a
    high = jnp.stack(turn_of(u))[:, :, None, :]
    v = 0.0
    for c, a in zip(box_coords(jnp.arange(64, dtype=jnp.int32), 2), slopes):
        v = v + ((c - 1.5) / 2.0 ** (LEVELS + 1))[:, None] * a
    return high, jnp.stack(turn_of(v))


def split(x):
    high = x.astype(jnp.bfloat16)
    return high, (x - high.astype(jnp.float32)).astype(jnp.bfloat16)


def dot(a, b):
    return jnp.dot(a, b, preferred_element_type=jnp.float32)


def forward_block(load, phase, table_ref, store, pb, kps, tgt):
    total = [None, None]
    for ep in range(4):
        parts = ([], [])
        for p in range(pb):
            a, b = load(p, ep), load(p, ep + 4)
            for kp in kps:
                (ca, sa), (cb, sb) = phase(p, ep, kp), phase(p, ep + 4, kp)
                for c, wa, wb in ((0, ca, cb), (1, sa, sb), (0, sa, sb), (1, ca, cb)):
                    va = [a[c][t] * wa[t] for t in range(2)]
                    vb = [b[c][t] * wb[t] for t in range(2)]
                    parts[0].append(jnp.concatenate([va[0] + vb[1], va[1] + vb[0]], axis=1))
                    parts[1].append(jnp.concatenate([va[0] - vb[1], va[1] - vb[0]], axis=1))
        for s in range(2):
            high, low = split(jnp.concatenate(parts[s], axis=0))
            table = table_ref[ep, s]
            r = dot(high, table) + dot(low, table)
            total[s] = r if total[s] is None else total[s] + r
    even, odd = (x[:, :128] + x[:, 128:] for x in total)
    n = 0
    for p in range(pb):
        for kp in kps:
            q = []
            for _ in range(4):
                rows = slice(n, n + tgt)
                q.append((even[rows] + odd[rows], even[rows] - odd[rows]))
                n += tgt
            for t in range(2):
                rc, si, rs, ci = (x[t] for x in q)
                store(p, kp, t, (rc - si, rs + ci))
                store(p, 7 - kp, t, (rc + si, ci - rs))


def phase_of(w_ref):
    def phase(s, kp):
        return [[w_ref[s, i : i + 1, t * 128 : t * 128 + 128] for t in range(2)] for i in (kp, 4 + kp)]

    return phase


def forward_level(load, w_ref, table_ref, y_ref, parents, tgt):
    pb, kb = min(parents, max(1, ROWS // (16 * tgt))), min(4, max(1, ROWS // (4 * tgt)))
    phase = phase_of(w_ref)
    for g in range(0, 4, kb):

        def body(i, carry):
            def store(p, k, t, values):
                for c in range(2):
                    y_ref[i * pb + p, c, t, k * tgt : (k + 1) * tgt] = values[c]

            source = lambda p, e: (i * pb + p) * 8 + e
            forward_block(
                lambda p, e: load(source(p, e)),
                lambda p, e, kp: phase(source(p, e), kp),
                table_ref, store, pb, range(g, g + kb), tgt,
            )
            return carry

        lax.fori_loop(0, parents // pb, body, 0)


def adjoint_block(load, phase, table_ref, store, pb, tgt):
    parts = ([], [])
    for p in range(pb):
        for kp in range(4):
            a, b = load(p, kp), load(p, 7 - kp)
            for c, sign in ((0, 1), (1, -1), (0, -1), (1, 1)):
                x = [a[c][t] + b[c][t] if sign > 0 else a[c][t] - b[c][t] for t in range(2)]
                parts[0].append(x[0] + x[1])
                parts[1].append(x[0] - x[1])
    rows = [jnp.concatenate(split(jnp.concatenate(x, axis=0)), axis=1) for x in parts]
    for ep in range(4):
        even, odd = (dot(rows[s], table_ref[ep, s, 0]) + dot(rows[s], table_ref[ep, s, 1]) for s in range(2))
        tiles = [slice(0, 128), slice(128, 256)]
        near = [even[:, t] + odd[:, t] for t in tiles]
        far = [even[:, t] - odd[:, t] for t in reversed(tiles)]
        for e, z in ((ep, near), (ep + 4, far)):
            n = 0
            for p in range(pb):
                out = [[None, None], [None, None]]
                for kp in range(4):
                    cs, sn = phase(p, e, kp)
                    for t in range(2):
                        q = [z[t][n + i * tgt : n + (i + 1) * tgt] for i in range(4)]
                        re, im = q[0] * cs[t] + q[1] * sn[t], q[3] * cs[t] - q[2] * sn[t]
                        out[0][t] = re if kp == 0 else out[0][t] + re
                        out[1][t] = im if kp == 0 else out[1][t] + im
                    n += 4 * tgt
                store(p, e, out)


def adjoint_level(y_ref, w_ref, table_ref, store, parents, tgt):
    tb = min(tgt, 32)
    pb, nt = min(parents, 32 // tb), tgt // tb
    phase = phase_of(w_ref)

    def body(i, carry):
        p0, t0 = (i // nt) * pb, pl.multiple_of((i % nt) * tb, 8)

        def load(p, k):
            rows = pl.ds(pl.multiple_of(k * tgt + t0, 8), tb)
            return [[y_ref[p0 + p, c, t, rows] for t in range(2)] for c in range(2)]

        source = lambda p, e: (p0 + p) * 8 + e
        adjoint_block(
            load,
            lambda p, e, kp: phase(source(p, e), kp),
            table_ref,
            lambda p, e, out: store(source(p, e), t0, tb, out),
            pb, tb,
        )
        return carry

    lax.fori_loop(0, (parents // pb) * nt, body, 0)


def to_lanes(x):
    out = []
    for n in (0, Q):
        far = [x[:, n + a : n + a + 36] for a in (180, 144, 108)] + [x[:, n : n + 20]]
        out.append([x[:, n : n + 128], jnp.concatenate(far, axis=1)])
    return out


def from_lanes(x):
    parts = []
    for c in range(2):
        parts += [x[c][0][:, :HALF]] + [x[c][1][:, a : a + 36] for a in (72, 36, 0)]
    return jnp.concatenate(parts, axis=1)


def turn(x, c, s, sign=1):
    if sign > 0:
        return [[x[0][t] * c[t] - x[1][t] * s[t] for t in range(2)], [x[0][t] * s[t] + x[1][t] * c[t] for t in range(2)]]
    return [[x[0][t] * c[t] + x[1][t] * s[t] for t in range(2)], [x[1][t] * c[t] - x[0][t] * s[t] for t in range(2)]]


def pack(groups):
    out, rest = [], []
    for x in groups:
        last = x[1][1]
        for i, y in enumerate((x[0][0], x[0][1], x[1][0])):
            out.append(jnp.concatenate([y[:, :HALF], last[:, 20 * i : 20 * i + 20]], axis=1))
        rest.append(last[:, 60:HALF])
    out.append(jnp.concatenate([rest[0], rest[0][:, :16], rest[1], rest[1][:, :16]], axis=1))
    return out


def unpack(x):
    groups = []
    for g in range(2):
        y = x[3 * g : 3 * g + 3]
        tail = x[6][:, 64 * g : 64 * g + 48]
        last = jnp.concatenate([v[:, HALF:] for v in y] + [tail, tail[:, :20]], axis=1)
        groups.append([[y[0], y[1]], [y[2], last]])
    return groups


def join_rows(groups):
    return [[jnp.concatenate([g[c][t] for g in groups], axis=0) for t in range(2)] for c in range(2)]


def forward_first(geo, x_ref, p0_ref, w0_ref, w1_ref, table_ref, o_ref, x_buf, y0_buf, y1_buf):
    D, m, T, slot = geo

    def first(i, carry):
        for j in range(4):
            s = i * 4 + j
            cs, sn = ([p0_ref[s, n, :, t * 128 : t * 128 + 128] for t in range(2)] for n in range(2))
            x = turn(to_lanes(x_ref[s]), cs, sn)
            for c in range(2):
                for t in range(2):
                    x_buf[s, c, t] = x[c][t]
        return carry

    lax.fori_loop(0, 16 * m, first, 0)
    read = lambda ref: lambda s: [[ref[s, c, t] for t in range(2)] for c in range(2)]
    forward_level(read(x_buf), w0_ref, table_ref, y0_buf, 8 * m, 8)
    forward_level(read(y0_buf), w1_ref, table_ref, y1_buf, m, 64)

    def send(i, carry):
        for r in range(4):
            d = i * 4 + r
            for p in range(m):
                groups = []
                for g in range(T // 8):
                    box = d * (T // 8) + g
                    rows = pl.ds((box % 8) * 8 + box // 8, 8, stride=64)
                    groups.append([[y1_buf[p, c, t, rows] for t in range(2)] for c in range(2)])
                for n, v in enumerate(pack(groups)):
                    o_ref[slot(d), p, n] = v
        return carry

    lax.fori_loop(0, D // 4, send, 0)


def forward_second(geo, x_ref, w2_ref, w3_ref, eh_ref, el_ref, table_ref, o_ref, y2_buf, y3_buf):
    D, m, T, slot = geo

    def load(s):
        i = slot(s // m)
        return join_rows(unpack([x_ref[i, s % m, n] for n in range(7)]))

    forward_level(load, w2_ref, table_ref, y2_buf, 8, T)
    read = lambda ref: lambda s: [[ref[s, c, t] for t in range(2)] for c in range(2)]
    forward_level(read(y2_buf), w3_ref, table_ref, y3_buf, 1, 8 * T)

    def last(a, carry):
        hc, hs = ([eh_ref[n, a, :, t * 128 : t * 128 + 128] for t in range(2)] for n in range(2))
        for k in range(8):
            rows = pl.ds(k * T + a, 8, stride=8 * T)
            x = [[y3_buf[0, c, t, rows] for t in range(2)] for c in range(2)]
            lc, ls = ([el_ref[n, k * 8 : k * 8 + 8, t * 128 : t * 128 + 128] for t in range(2)] for n in range(2))
            x = turn(turn(x, lc, ls, -1), hc, hs, -1)
            o_ref[pl.ds(pl.multiple_of(a * 64 + k * 8, 8), 8), :] = from_lanes(x)
        return carry

    lax.fori_loop(0, T, last, 0)


def adjoint_first(geo, y_ref, w2_ref, w3_ref, eh_ref, el_ref, table_ref, o_ref, y_buf, x3_buf):
    D, m, T, slot = geo

    def first(a, carry):
        hc, hs = ([eh_ref[n, a, :, t * 128 : t * 128 + 128] for t in range(2)] for n in range(2))
        for k in range(8):
            x = to_lanes(y_ref[pl.ds(pl.multiple_of(a * 64 + k * 8, 8), 8), :])
            lc, ls = ([el_ref[n, k * 8 : k * 8 + 8, t * 128 : t * 128 + 128] for t in range(2)] for n in range(2))
            x = turn(turn(x, lc, ls), hc, hs)
            for c in range(2):
                for t in range(2):
                    y_buf[0, c, t, pl.ds(k * T + a, 8, stride=8 * T)] = x[c][t]
        return carry

    lax.fori_loop(0, T, first, 0)

    def keep(s, t0, tb, out):
        for c in range(2):
            for t in range(2):
                x3_buf[s, c, t, pl.ds(t0, tb)] = out[c][t]

    adjoint_level(y_buf, w3_ref, table_ref, keep, 1, 8 * T)

    def send(s, t0, tb, out):
        groups = [[[out[c][t][g * 8 : g * 8 + 8] for t in range(2)] for c in range(2)] for g in range(T // 8)]
        for n, v in enumerate(pack(groups)):
            o_ref[slot(s // m), s % m, n] = v

    adjoint_level(x3_buf, w2_ref, table_ref, send, 8, T)


def adjoint_second(geo, y_ref, p0_ref, w0_ref, w1_ref, table_ref, o_ref, y_buf, x1_buf, x0_buf):
    D, m, T, slot = geo

    def first(i, carry):
        for r in range(4):
            d = i * 4 + r
            for p in range(m):
                for g, x in enumerate(unpack([y_ref[slot(d), p, n] for n in range(7)])):
                    box = d * (T // 8) + g
                    rows = pl.ds((box % 8) * 8 + box // 8, 8, stride=64)
                    for c in range(2):
                        for t in range(2):
                            y_buf[p, c, t, rows] = x[c][t]
        return carry

    lax.fori_loop(0, D // 4, first, 0)

    def keep(s, t0, tb, out):
        for c in range(2):
            for t in range(2):
                x1_buf[s, c, t, pl.ds(t0, tb)] = out[c][t]

    adjoint_level(y_buf, w1_ref, table_ref, keep, m, 64)

    def last(s, t0, tb, out):
        cs, sn = ([p0_ref[s, n, :, t * 128 : t * 128 + 128] for t in range(2)] for n in range(2))
        out = turn(out, cs, sn, -1)
        for c in range(2):
            for t in range(2):
                x0_buf[c, t, pl.ds(pl.multiple_of(s * 8, 8), 8)] = out[c][t]

    adjoint_level(x1_buf, w0_ref, table_ref, last, 8 * m, 8)

    def turn_rows(i, carry):
        for a in range(8):
            rows = pl.ds(i * 64 + a, 8, stride=8)
            x = [[x0_buf[c, t, rows] for t in range(2)] for c in range(2)]
            o_ref[a, pl.ds(pl.multiple_of(i * 8, 8), 8), :] = from_lanes(x)
        return carry

    lax.fori_loop(0, 8 * m, turn_rows, 0)


def vmem_call(kernel, out_shape, scratch, *args):
    spec = pl.BlockSpec(memory_space=pltpu.VMEM)
    return pl.pallas_call(
        kernel,
        in_specs=[spec] * len(args),
        out_specs=spec,
        out_shape=jax.ShapeDtypeStruct(out_shape, jnp.float32),
        scratch_shapes=[pltpu.VMEM(s, jnp.float32) for s in scratch],
        compiler_params=pltpu.CompilerParams(vmem_limit_bytes=56 * 1024 * 1024),
    )(*args)


def one_exchange_shards(forward_weights, adjoint_weights, medium):
    nx, ny = lax.axis_size("sx"), lax.axis_size("sy")
    ix, iy = lax.axis_index("sx"), lax.axis_index("sy")
    D, S, R = nx * ny, forward_weights.shape[0], adjoint_weights.shape[0]
    m, T = S // 64, R // 64
    natural = lambda d: d
    swapped = lambda d: (d % nx) * ny + d // nx
    swapped_back = lambda d: (d % ny) * nx + d // ny
    src, tgt = (iy * nx + ix) * S, (ix * ny + iy) * R
    forward_table, adjoint_table = forward_parity_table(), adjoint_parity_table()
    p0 = first_phase(src, S, medium)
    w0 = level_phase(src, S, 0, medium)
    w1 = level_phase(src // 8, S // 8, 1, medium)
    w2 = level_phase(jnp.int32(0), 64, 2, medium)
    w3 = level_phase(jnp.int32(0), 8, 3, medium)
    eh, el = last_phase(tgt, R, medium)
    wire = (D, m, 7, 8, 128)
    data = lambda s, t: (s, 2, 2, t, 128)
    x = vmem_call(
        lambda *a: forward_first((D, m, T, natural), *a), wire,
        [data(S, 8), data(8 * m, 64), data(m, 512)], forward_weights, p0, w0, w1, forward_table,
    )
    x = lax.all_to_all(x, ("sx", "sy"), split_axis=0, concat_axis=0, tiled=True)
    y = vmem_call(
        lambda *a: adjoint_first((D, m, T, swapped), *a), wire,
        [data(1, 64 * T), data(8, 8 * T)], adjoint_weights, w2, w3, eh, el, adjoint_table,
    )
    y = lax.all_to_all(y, ("sx", "sy"), split_axis=0, concat_axis=0, tiled=True)
    f = vmem_call(
        lambda *a: forward_second((D, m, T, swapped), *a), (R, 2 * Q),
        [data(8, 8 * T), data(1, 64 * T)], x, w2, w3, eh, el, forward_table,
    )
    b = vmem_call(
        lambda *a: adjoint_second((D, m, T, natural), *a), (8, S, 2 * Q),
        [data(m, 512), data(8 * m, 64), (2, 2, S * 8, 128)], y, p0, w0, w1, adjoint_table,
    )
    return f, b


def shards(forward_weights, adjoint_weights, medium):
    devices = lax.axis_size("sx") * lax.axis_size("sy")
    S, R = forward_weights.shape[0], adjoint_weights.shape[0]
    one = S % 64 == 0 and (S // 64) * devices == 64 and R == 1024 and forward_weights.shape[2] == 2 * Q
    return (one_exchange_shards if one else general_shards)(forward_weights, adjoint_weights, medium)


def solution(mesh):
    in_specs = (P(("sy", "sx"), None, None), P(("sx", "sy"), None), P())
    out_specs = (P(("sx", "sy"), None), P(None, ("sy", "sx"), None))
    return jax.shard_map(shards, mesh=mesh, in_specs=in_specs, out_specs=out_specs, check_vma=False)
```

```python
import math

import jax
import jax.numpy as jnp
import ml_dtypes
import numpy as np
from jax import lax
from jax.experimental import pallas as pl
from jax.experimental.pallas import tpu as pltpu
from jax.sharding import PartitionSpec as P

ORDER = 6
LEVELS = 4
Q = 216
band = 8.0


def cheb_points(n):
    return np.array([(1.0 - math.cos((2 * i + 1) * math.pi / (2 * n))) / 2.0 for i in range(n)])


def child_table(n):
    g = cheb_points(n)
    halves = []
    for bit in range(2):
        m = np.ones((n, n))
        for r in range(n):
            w = (g[r] + bit) / 2.0
            for c in range(n):
                for o in range(n):
                    if o != c:
                        m[r, c] *= (w - g[o]) / (g[c] - g[o])
        halves.append(m)
    return np.stack(
        [np.kron(np.kron(halves[e // 4], halves[e // 2 % 2]), halves[e % 2]) for e in range(8)]
    )


def split_table(table):
    high = table.astype(ml_dtypes.bfloat16)
    low = (table - high.astype(np.float64)).astype(ml_dtypes.bfloat16)
    return jnp.asarray(high), jnp.asarray(low)


def box_coords(index, groups):
    coords = [jnp.zeros_like(index) for _ in range(3)]
    for group in range(groups):
        digit = index // 8 ** (groups - 1 - group) % 8
        bits = (digit // 4, digit // 2 % 2, digit % 2)
        coords = [c * 2 + b for c, b in zip(coords, bits)]
    return [c.astype(jnp.float32) for c in coords]


def point_slopes(src_off, count, groups, medium):
    side = band / float(2**groups)
    g = cheb_points(ORDER).astype(np.float32)
    grid = (np.repeat(g, ORDER * ORDER), np.tile(np.repeat(g, ORDER), ORDER), np.tile(g, ORDER**2))
    corner = box_coords(src_off + jnp.arange(count, dtype=jnp.int32), groups)
    pts = [side * (c[:, None] + o[None, :]) for c, o in zip(corner, grid)]
    radius = jnp.sqrt(pts[0] * pts[0] + pts[1] * pts[1] + pts[2] * pts[2])
    return [p + medium[d + 1] * radius for d, p in enumerate(pts)], medium[0] * radius


def turn_of(u):
    half = jnp.round(2.0 * u)
    y = (2.0 * math.pi) * (u - 0.5 * half)
    sign = 1.0 - 2.0 * (half - 2.0 * jnp.floor(0.5 * half))
    z = y * y
    s = jnp.float32(-1.0 / math.factorial(11))
    for n in (9, 7, 5, 3, 1):
        s = s * z + (1.0 if n % 4 == 1 else -1.0) / math.factorial(n)
    c = jnp.float32(1.0 / math.factorial(12))
    for n in (10, 8, 6, 4, 2, 0):
        c = c * z + (1.0 if n % 4 == 0 else -1.0) / math.factorial(n)
    return sign * c, sign * (s * y)


def pair_phase(src_off, src_count, src_groups, tgt_off, tgt_count, tgt_groups, medium):
    slopes, base = point_slopes(src_off, src_count, src_groups, medium)
    coords = box_coords(tgt_off + jnp.arange(tgt_count, dtype=jnp.int32), tgt_groups)
    u = base[:, None, :]
    for c, a in zip(coords, slopes):
        u = u + ((c + 0.5) / float(2**tgt_groups))[None, :, None] * a[:, None, :]
    return turn_of(u)


def child_phase(src_off, src_count, level, medium):
    slopes, _ = point_slopes(src_off, src_count, LEVELS - level, medium)
    k = np.arange(8)
    u = 0.0
    for bits, a in zip((k // 4, k // 2 % 2, k % 2), slopes):
        step = ((bits - 0.5) / 2.0 ** (level + 2)).astype(np.float32)
        u = u + step[None, :, None] * a[:, None, :]
    return jnp.stack(turn_of(u), axis=1)


def dot3(x, high, low):
    x_high = x.astype(jnp.bfloat16)
    x_low = (x - x_high.astype(jnp.float32)).astype(jnp.bfloat16)
    dot = lambda a, b: jnp.dot(a, b, preferred_element_type=jnp.float32)
    return dot(x_high, high) + dot(x_high, low) + dot(x_low, high)


def forward_kernel(x_ref, w_ref, high_ref, low_ref, o_ref):
    pb, _, _, tb, q = o_ref.shape[0], 2, 8, o_ref.shape[3], o_ref.shape[4]

    def step(e, acc):
        parts = []
        for p in range(pb):
            re, im = x_ref[p, e, 0], x_ref[p, e, 1]
            w_re, w_im = w_ref[p, e, 0], w_ref[p, e, 1]
            res = [re * w_re[k : k + 1] - im * w_im[k : k + 1] for k in range(8)]
            ims = [re * w_im[k : k + 1] + im * w_re[k : k + 1] for k in range(8)]
            parts += res + ims
        return acc + dot3(jnp.concatenate(parts, axis=0), high_ref[e], low_ref[e])

    acc = lax.fori_loop(0, 8, step, jnp.zeros((pb * 16 * tb, q), jnp.float32))
    o_ref[...] = acc.reshape(o_ref.shape)


def adjoint_kernel(y_ref, w_ref, high_ref, low_ref, o_ref):
    sb, tb, q = y_ref.shape[0], y_ref.shape[3], y_ref.shape[4]
    rows = y_ref[...].reshape(sb * 16 * tb, q)

    def step(e, carry):
        z = dot3(rows, high_ref[e], low_ref[e]).reshape(sb, 2, 8, tb, q)
        for s in range(sb):
            w_re, w_im = w_ref[s, e, 0], w_ref[s, e, 1]
            out_re = jnp.zeros((tb, q), jnp.float32)
            out_im = jnp.zeros((tb, q), jnp.float32)
            for k in range(8):
                re, im = z[s, 0, k], z[s, 1, k]
                c, d = w_re[k : k + 1], w_im[k : k + 1]
                out_re += re * c + im * d
                out_im += im * c - re * d
            o_ref[s, e, 0] = out_re
            o_ref[s, e, 1] = out_im
        return carry

    lax.fori_loop(0, 8, step, 0)


def blocks(count, tgt):
    tb = min(tgt, 32)
    return math.gcd(count, max(1, 32 // tb)), tb


def level_call(kernel, operand, phase, tables, out_shape):
    count, tgt, q = operand.shape[0], operand.shape[3], operand.shape[4]
    cb, tb = blocks(count, tgt)
    spec = lambda: pl.BlockSpec((cb, operand.shape[1], operand.shape[2], tb, q), lambda i, j: (i, 0, 0, j, 0))
    return pl.pallas_call(
        kernel,
        grid=(count // cb, tgt // tb),
        in_specs=[
            spec(),
            pl.BlockSpec((cb,) + phase.shape[1:], lambda i, j: (i, 0, 0, 0, 0)),
            pl.BlockSpec(tables[0].shape, lambda i, j: (0, 0, 0)),
            pl.BlockSpec(tables[1].shape, lambda i, j: (0, 0, 0)),
        ],
        out_specs=pl.BlockSpec((cb, out_shape[1], out_shape[2], tb, q), lambda i, j: (i, 0, 0, j, 0)),
        out_shape=jax.ShapeDtypeStruct(out_shape, jnp.float32),
        compiler_params=pltpu.CompilerParams(vmem_limit_bytes=56 * 1024 * 1024),
    )(operand, phase, *tables)


def general_forward_level(x, src_off, level, medium, tables):
    count, _, tgt, q = x.shape
    phase = child_phase(src_off, count, level, medium).reshape(count // 8, 8, 2, 8, q)
    out = level_call(
        forward_kernel, x.reshape(count // 8, 8, 2, tgt, q), phase, tables, (count // 8, 2, 8, tgt, q)
    )
    return out.swapaxes(2, 3).reshape(count // 8, 2, tgt * 8, q)


def general_adjoint_level(y, src_off, level, medium, tables):
    count, _, tgt, q = y.shape
    phase = child_phase(src_off * 8, count * 8, level, medium).reshape(count, 8, 2, 8, q)
    operand = y.reshape(count, 2, tgt // 8, 8, q).swapaxes(2, 3)
    out = level_call(adjoint_kernel, operand, phase, tables, (count, 8, 2, tgt // 8, q))
    return out.reshape(count * 8, 2, tgt // 8, q)


def general_shards(forward_weights, adjoint_weights, medium):
    table = child_table(ORDER) / math.sqrt(8.0)
    forward_tables = split_table(table)
    adjoint_tables = split_table(table.transpose(0, 2, 1))
    sizes = {a: lax.axis_size(a) for a in ("sx", "sy")}
    index = {a: lax.axis_index(a) for a in ("sx", "sy")}
    local_sources = forward_weights.shape[0]
    shots = forward_weights.shape[2] // (2 * Q)
    plan = []
    remaining = ["sx", "sy"]
    width = local_sources
    for _ in range(LEVELS):
        while width < 8:
            axis = remaining.pop(0)
            plan.append(axis)
            width *= sizes[axis]
        plan.append("level")
        width //= 8

    f_in = forward_weights.reshape(local_sources, -1, 2, shots, Q)
    b_in = adjoint_weights.reshape(adjoint_weights.shape[0], 2, shots, Q)
    f_src = (index["sy"] * sizes["sx"] + index["sx"]) * local_sources
    b_tgt = (index["sx"] * sizes["sy"] + index["sy"]) * adjoint_weights.shape[0]
    f_outs, b_outs = [], []
    for shot in range(shots):
        src, tgt, level = f_src, jnp.int32(0), 0
        re, im = f_in[:, :, 0, shot], f_in[:, :, 1, shot]
        c, s = pair_phase(src, re.shape[0], LEVELS, tgt, re.shape[1], 1, medium)
        x = jnp.stack([re * c - im * s, re * s + im * c], axis=1)
        for op in plan:
            if op == "level":
                x = general_forward_level(x, src, level, medium, forward_tables)
                src, tgt, level = src // 8, tgt * 8, level + 1
            else:
                n = sizes[op]
                count, _, width, _ = x.shape
                x = x.reshape(count, 2, n, width // n, Q).transpose(2, 0, 1, 3, 4)
                x = lax.all_to_all(x, op, split_axis=0, concat_axis=0, tiled=True)
                x = x.reshape(n * count, 2, width // n, Q)
                src = src - index[op] * count
                tgt = tgt + index[op] * (width // n)
        c, s = pair_phase(src, x.shape[0], LEVELS - level, tgt, x.shape[2], level + 1, medium)
        re, im = x[:, 0], x[:, 1]
        f_outs.append((re * c + im * s, im * c - re * s))
        src, tgt, level = jnp.int32(0), b_tgt, LEVELS
        re, im = b_in[None, :, 0, shot], b_in[None, :, 1, shot]
        c, s = pair_phase(src, 1, 0, tgt, re.shape[1], LEVELS + 1, medium)
        y = jnp.stack([re * c - im * s, re * s + im * c], axis=1)
        for op in reversed(plan):
            if op == "level":
                y = general_adjoint_level(y, src, level - 1, medium, adjoint_tables)
                src, tgt, level = src * 8, tgt // 8, level - 1
            else:
                n = sizes[op]
                count, _, width, _ = y.shape
                y = y.reshape(n, count // n, 2, width, Q)
                y = lax.all_to_all(y, op, split_axis=0, concat_axis=0, tiled=True)
                y = y.transpose(1, 2, 0, 3, 4).reshape(count // n, 2, n * width, Q)
                src = src + index[op] * (count // n)
                tgt = tgt - index[op] * width
        c, s = pair_phase(src, y.shape[0], LEVELS, tgt, y.shape[2], 1, medium)
        re, im = y[:, 0], y[:, 1]
        b_outs.append((re * c + im * s, im * c - re * s))
    f = jnp.stack([jnp.stack([o[i][0] for o in f_outs], axis=1) for i in range(2)], axis=1)
    b = jnp.stack([jnp.stack([o[i].swapaxes(0, 1) for o in b_outs], axis=2) for i in range(2)], axis=2)
    return f.reshape(f.shape[0], -1), b.reshape(b.shape[0], b.shape[1], -1)


HALF = Q // 2
ROWS = 512


def lane_points():
    t = np.arange(HALF)
    return t, (ORDER - 1 - t // ORDER**2) * ORDER**2 + t % ORDER**2


def parity_tables():
    t, m = lane_points()
    table = child_table(ORDER) / math.sqrt(8.0)
    out = np.zeros((4, 2, 256, 128))
    for e in range(4):
        rows = np.zeros((256, Q))
        rows[:HALF] = table[e][t]
        rows[128 : 128 + HALF] = table[e][m]
        for s, sign in enumerate((1.0, -1.0)):
            out[e, s, :, :HALF] = 0.5 * (rows[:, t] + sign * rows[:, m])
    high = out.astype(ml_dtypes.bfloat16)
    return high, (out - high.astype(np.float64)).astype(ml_dtypes.bfloat16)


def forward_parity_table():
    high, low = parity_tables()
    return jnp.asarray(np.concatenate([high, low], axis=-1))


def adjoint_parity_table():
    parts = [np.concatenate([x.swapaxes(-1, -2)] * 2, axis=2) for x in parity_tables()]
    return jnp.asarray(np.stack(parts, axis=2))


def split(x):
    high = x.astype(jnp.bfloat16)
    return high, (x - high.astype(jnp.float32)).astype(jnp.bfloat16)


def dot(a, b):
    return jnp.dot(a, b, preferred_element_type=jnp.float32)


def forward_block(load, phase, table_ref, store, pb, kps, tgt):
    total = [None, None]
    for ep in range(4):
        parts = ([], [])
        for p in range(pb):
            a, b = load(p, ep), load(p, ep + 4)
            for kp in kps:
                (ca, sa), (cb, sb) = phase(p, ep, kp), phase(p, ep + 4, kp)
                for c, wa, wb in ((0, ca, cb), (1, sa, sb), (0, sa, sb), (1, ca, cb)):
                    va = [a[c][t] * wa[t] for t in range(2)]
                    vb = [b[c][t] * wb[t] for t in range(2)]
                    parts[0].append(jnp.concatenate([va[0] + vb[1], va[1] + vb[0]], axis=1))
                    parts[1].append(jnp.concatenate([va[0] - vb[1], va[1] - vb[0]], axis=1))
        for s in range(2):
            high, low = split(jnp.concatenate(parts[s], axis=0))
            table = table_ref[ep, s]
            r = dot(high, table) + dot(low, table)
            total[s] = r if total[s] is None else total[s] + r
    even, odd = (x[:, :128] + x[:, 128:] for x in total)
    n = 0
    for p in range(pb):
        for kp in kps:
            q = []
            for _ in range(4):
                rows = slice(n, n + tgt)
                q.append((even[rows] + odd[rows], even[rows] - odd[rows]))
                n += tgt
            for t in range(2):
                rc, si, rs, ci = (x[t] for x in q)
                store(p, kp, t, (rc - si, rs + ci))
                store(p, 7 - kp, t, (rc + si, ci - rs))


def phase_of(w_ref, first=0):
    def phase(s, kp):
        return [[w_ref[t, first + s, i : i + 1] for t in range(2)] for i in (kp, 4 + kp)]

    return phase


def forward_level(load, phase, table_ref, y_ref, parents, tgt):
    pb, kb = min(parents, max(1, ROWS // (16 * tgt))), min(4, max(1, ROWS // (4 * tgt)))
    for g in range(0, 4, kb):

        def body(i, carry):
            def store(p, k, t, values):
                for c in range(2):
                    y_ref[i * pb + p, c, t, k * tgt : (k + 1) * tgt] = values[c]

            source = lambda p, e: (i * pb + p) * 8 + e
            forward_block(
                lambda p, e: load(source(p, e)),
                lambda p, e, kp: phase(source(p, e), kp),
                table_ref, store, pb, range(g, g + kb), tgt,
            )
            return carry

        lax.fori_loop(0, parents // pb, body, 0)


def adjoint_block(load, phase, table_ref, store, pb, tgt):
    parts = ([], [])
    for p in range(pb):
        for kp in range(4):
            a, b = load(p, kp), load(p, 7 - kp)
            for c, sign in ((0, 1), (1, -1), (0, -1), (1, 1)):
                x = [a[c][t] + b[c][t] if sign > 0 else a[c][t] - b[c][t] for t in range(2)]
                parts[0].append(x[0] + x[1])
                parts[1].append(x[0] - x[1])
    rows = [jnp.concatenate(split(jnp.concatenate(x, axis=0)), axis=1) for x in parts]
    for ep in range(4):
        even, odd = (dot(rows[s], table_ref[ep, s, 0]) + dot(rows[s], table_ref[ep, s, 1]) for s in range(2))
        tiles = [slice(0, 128), slice(128, 256)]
        near = [even[:, t] + odd[:, t] for t in tiles]
        far = [even[:, t] - odd[:, t] for t in reversed(tiles)]
        for e, z in ((ep, near), (ep + 4, far)):
            n = 0
            for p in range(pb):
                out = [[None, None], [None, None]]
                for kp in range(4):
                    cs, sn = phase(p, e, kp)
                    for t in range(2):
                        q = [z[t][n + i * tgt : n + (i + 1) * tgt] for i in range(4)]
                        re, im = q[0] * cs[t] + q[1] * sn[t], q[3] * cs[t] - q[2] * sn[t]
                        out[0][t] = re if kp == 0 else out[0][t] + re
                        out[1][t] = im if kp == 0 else out[1][t] + im
                    n += 4 * tgt
                store(p, e, out)


def adjoint_level(y_ref, phase, table_ref, store, parents, tgt):
    tb = min(tgt, 32)
    pb, nt = min(parents, 32 // tb), tgt // tb

    def body(i, carry):
        p0, t0 = (i // nt) * pb, pl.multiple_of((i % nt) * tb, 8)

        def load(p, k):
            rows = pl.ds(pl.multiple_of(k * tgt + t0, 8), tb)
            return [[y_ref[p0 + p, c, t, rows] for t in range(2)] for c in range(2)]

        source = lambda p, e: (p0 + p) * 8 + e
        adjoint_block(
            load,
            lambda p, e, kp: phase(source(p, e), kp),
            table_ref,
            lambda p, e, out: store(source(p, e), t0, tb, out),
            pb, tb,
        )
        return carry

    lax.fori_loop(0, (parents // pb) * nt, body, 0)


def turn(x, c, s, sign=1):
    if sign > 0:
        return [[x[0][t] * c[t] - x[1][t] * s[t] for t in range(2)], [x[0][t] * s[t] + x[1][t] * c[t] for t in range(2)]]
    return [[x[0][t] * c[t] + x[1][t] * s[t] for t in range(2)], [x[1][t] * c[t] - x[0][t] * s[t] for t in range(2)]]


def pack(groups):
    out, rest = [], []
    for x in groups:
        last = x[1][1]
        for i, y in enumerate((x[0][0], x[0][1], x[1][0])):
            out.append(jnp.concatenate([y[:, :HALF], last[:, 20 * i : 20 * i + 20]], axis=1))
        rest.append(last[:, 60:HALF])
    out.append(jnp.concatenate([rest[0], rest[0][:, :16], rest[1], rest[1][:, :16]], axis=1))
    return out


def unpack(x):
    groups = []
    for g in range(2):
        y = x[3 * g : 3 * g + 3]
        tail = x[6][:, 64 * g : 64 * g + 48]
        last = jnp.concatenate([v[:, HALF:] for v in y] + [tail, tail[:, :20]], axis=1)
        groups.append([[y[0], y[1]], [y[2], last]])
    return groups


def join_rows(groups):
    return [[jnp.concatenate([g[c][t] for g in groups], axis=0) for t in range(2)] for c in range(2)]


def grid_rows():
    t, m = lane_points()
    g = cheb_points(ORDER).astype(np.float32)
    full = (np.repeat(g, ORDER * ORDER), np.tile(np.repeat(g, ORDER), ORDER), np.tile(g, ORDER**2))
    out = np.zeros((8, 128), np.float32)
    for d in range(3):
        out[2 * d, :HALF], out[2 * d + 1, :HALF] = full[d][t], full[d][m]
    return jnp.asarray(out)


def bits_of(index, groups):
    coords = [jnp.zeros_like(index) for _ in range(3)]
    for group in range(groups):
        digit = (index >> (3 * (groups - 1 - group))) & 7
        coords = [c * 2 + ((digit >> b) & 1) for c, b in zip(coords, (2, 1, 0))]
    return [c.astype(jnp.float32) for c in coords]


def slopes_of(index, groups, t, grid_ref, med):
    side = band / float(2**groups)
    pts = [side * (c + grid_ref[2 * d + t : 2 * d + t + 1]) for d, c in enumerate(bits_of(index, groups))]
    radius = jnp.sqrt(pts[0] * pts[0] + pts[1] * pts[1] + pts[2] * pts[2])
    return [p + med[d + 1] * radius for d, p in enumerate(pts)], med[0] * radius


def rows_index():
    return lax.broadcasted_iota(jnp.int32, (8, 128), 0)


def fill_level(w_ref, flat_ref, first, count, level, grid_ref, med, p0_ref=None):
    def body(i, carry):
        index = first + i * 8 + rows_index()
        for t in range(2):
            slopes, base = slopes_of(index, LEVELS - level, t, grid_ref, med)
            if p0_ref is not None:
                bc, bs = turn_of(base + 0.5 * (slopes[0] + slopes[1] + slopes[2]))
            for kp in range(4):
                u = 0.0
                for bit, a in zip((kp // 4, kp // 2 % 2, kp % 2), slopes):
                    u = u + ((bit - 0.5) / 2.0 ** (level + 2)) * a
                c, s = turn_of(u)
                flat_ref[t, pl.ds(i * 64 + kp, 8, stride=8)] = c
                flat_ref[t, pl.ds(i * 64 + 4 + kp, 8, stride=8)] = s
                if p0_ref is not None:
                    c2, s2 = c * c - s * s, 2.0 * c * s
                    cc, ss, cs, sc = bc * c2, bs * s2, bc * s2, bs * c2
                    for k, v, w in ((kp, cc - ss, cs + sc), (7 - kp, cc + ss, sc - cs)):
                        p0_ref[0, t, pl.ds(i * 64 + k, 8, stride=8)] = v
                        p0_ref[1, t, pl.ds(i * 64 + k, 8, stride=8)] = w
        for t in range(2):
            for j in range(8):
                w_ref[t, i * 8 + j] = flat_ref[t, pl.ds(pl.multiple_of(i * 64 + j * 8, 8), 8)]
        return carry

    lax.fori_loop(0, count // 8, body, 0)


def take_tiles(read):
    out = []
    for n in (0, Q):
        far = [read(n + a, n + a + 36) for a in (180, 144, 108)] + [read(n, n + 20)]
        out.append([read(n, n + 128).T, jnp.concatenate(far, axis=0).T])
    return out


def put_tiles(x, write):
    for c, n in ((0, 0), (1, Q)):
        near, far = x[c][0].T, x[c][1].T
        write(n, near[:HALF])
        for i, a in enumerate((72, 36, 0)):
            write(n + HALF + 36 * i, far[a : a + 36])


def load_pairs(ref, *index):
    return [[ref[(*index, c, t)] for t in range(2)] for c in range(2)]


def load_rows(ref, rows):
    return [[ref[c, t, rows] for t in range(2)] for c in range(2)]


def whole_kernel(
    geo, med, fw_ref, aw_hbm, grid_ref, ft_ref, at_hbm, fo_ref, ao_ref,
    aw_ref, at_ref, xa, xb, xc, xd, xe, p0, w0, w1, w2, w3, flat, el, send_f, send_a, recv_f, recv_a,
    send_sem, recv_sem, load_sem,
):
    D, m, T, nx, ny = geo
    ix, iy = lax.axis_index("sx"), lax.axis_index("sy")
    me_s, me_t = iy * nx + ix, ix * ny + iy
    med = [med[i] for i in range(4)]
    mesh_id = pl.DeviceIdType.MESH
    at_target = lambda d: (d // ny, lax.rem(d, ny))
    at_source = lambda d: (lax.rem(d, nx), d // nx)
    barrier = pltpu.get_barrier_semaphore()

    def greet(r, carry):
        pl.semaphore_signal(barrier, inc=1, device_id=at_target(lax.rem(me_t + r, D)), device_id_type=mesh_id)
        return carry

    lax.fori_loop(1, D, greet, 0)
    loads = [pltpu.make_async_copy(aw_hbm, aw_ref, load_sem.at[0]), pltpu.make_async_copy(at_hbm, at_ref, load_sem.at[1])]
    for copy in loads:
        copy.start()

    mine = (me_t, me_s)
    slot = (me_s, me_t)
    send, recv = (send_f, send_a), (recv_f, recv_a)
    place = (at_target, at_source)

    def block_copy(w, p, d, q):
        return pltpu.make_async_remote_copy(
            src_ref=send[w].at[p, d], dst_ref=recv[w].at[p, q],
            send_sem=send_sem.at[w, p, d], recv_sem=recv_sem.at[w, p, q],
            device_id=place[w](d), device_id_type=mesh_id,
        )

    def over_others(first, step):
        def body(r, carry):
            step(lax.rem(first + r, D))
            return carry

        lax.fori_loop(1, D, body, 0)

    def start_all(w, p):
        over_others(mine[w], lambda d: block_copy(w, p, d, slot[w]).start())
        for n in range(7):
            recv[w][p, slot[w], n] = send[w][p, mine[w], n]

    def wait_all(w, p):
        over_others(slot[w], lambda q: block_copy(w, p, q, q).wait_recv())

    def drain_all(w, p):
        over_others(mine[w], lambda d: block_copy(w, p, d, slot[w]).wait_send())

    src = me_s * (64 * m)
    fill_level(w0, flat, src, 64 * m, 0, grid_ref, med, p0)
    fill_level(w1, flat, src // 8, 8 * m, 1, grid_ref, med)

    def bring(a, carry):
        x = take_tiles(lambda i, j: fw_ref[a, i:j])
        for c in range(2):
            for t in range(2):
                for i in range(8 * m):
                    xa[c, t, pl.ds(i * 64 + a, 8, stride=8)] = x[c][t][i * 8 : i * 8 + 8]
        return carry

    lax.fori_loop(0, 8, bring, 0)
    pl.semaphore_wait(barrier, D - 1)

    def rows_of(ref, s):
        return load_rows(ref, pl.ds(pl.multiple_of(s * 8, 8), 8))

    def forward_half(p, carry):
        def load(s):
            cs, sn = rows_of(p0, p * 64 + s)
            return turn(rows_of(xa, p * 64 + s), cs, sn)

        forward_level(load, phase_of(w0, p * 64), ft_ref, xb, 8, 8)
        forward_level(lambda s: load_pairs(xb, s), phase_of(w1, p * 8), ft_ref, xc, 1, 64)

        def fill(i, carry):
            for r in range(4):
                d = i * 4 + r
                groups = []
                for g in range(T // 8):
                    box = d * (T // 8) + g
                    groups.append(load_rows(xc.at[0], pl.ds((box % 8) * 8 + box // 8, 8, stride=64)))
                for n, v in enumerate(pack(groups)):
                    send_f[p, d, n] = v
            return carry

        lax.fori_loop(0, D // 4, fill, 0)
        start_all(0, p)
        return carry

    lax.fori_loop(0, m, forward_half, 0)

    fill_level(w2, flat, 0, 64, 2, grid_ref, med)
    fill_level(w3, flat, 0, 8, 3, grid_ref, med)
    zero = jnp.zeros((8, 128), jnp.int32)

    def low(k, carry):
        for t in range(2):
            v = 0.0
            for c, a in zip(bits_of(k * 8 + rows_index(), 2), slopes_of(zero, 0, t, grid_ref, med)[0]):
                v = v + ((c - 1.5) / 2.0 ** (LEVELS + 1)) * a
            cs, sn = turn_of(v)
            rows = pl.ds(pl.multiple_of(k * 8, 8), 8)
            el[0, t, rows] = cs
            el[1, t, rows] = sn
        return carry

    lax.fori_loop(0, 8, low, 0)

    def high_phase(a):
        out = ([], [])
        for t in range(2):
            slopes, u = slopes_of(zero, 0, t, grid_ref, med)
            for c, s in zip(bits_of(zero + (me_t * T + a), LEVELS - 1), slopes):
                u = u + ((c + 0.5) / 2.0 ** (LEVELS - 1)) * s
            cs, sn = turn_of(u)
            out[0].append(cs)
            out[1].append(sn)
        return out

    for copy in loads:
        copy.wait()

    def take_targets(b, carry):
        lanes = pl.ds(pl.multiple_of(b * 128, 128), 128)
        x = take_tiles(lambda i, j: aw_ref[i:j, lanes])
        for h in range(2):
            a = b * 2 + h
            hc, hs = high_phase(a)
            for k in range(8):
                rows = slice(h * 64 + k * 8, h * 64 + k * 8 + 8)
                lc, ls = load_rows(el, slice(k * 8, k * 8 + 8))
                y = turn(turn([[x[c][t][rows] for t in range(2)] for c in range(2)], lc, ls), hc, hs)
                for c in range(2):
                    for t in range(2):
                        xd[0, c, t, pl.ds(k * T + a, 8, stride=8 * T)] = y[c][t]
        return carry

    lax.fori_loop(0, T // 2, take_targets, 0)

    def keep_in(ref):
        def store(s, t0, tb, out):
            for c in range(2):
                for t in range(2):
                    ref[s, c, t, pl.ds(t0, tb)] = out[c][t]

        return store

    def fill_back(s, t0, tb, out):
        groups = [[[out[c][t][g * 8 : g * 8 + 8] for t in range(2)] for c in range(2)] for g in range(T // 8)]
        for n, v in enumerate(pack(groups)):
            send_a[lax.rem(s, m), s // m, n] = v

    adjoint_level(xd, phase_of(w3), at_ref, keep_in(xe), 1, 8 * T)
    adjoint_level(xe, phase_of(w2), at_ref, fill_back, 8, T)
    for p in range(m):
        start_all(1, p)

    for p in range(m):
        wait_all(0, p)

    def arrived(s):
        return join_rows(unpack([recv_f[lax.rem(s, m), s // m, n] for n in range(7)]))

    forward_level(arrived, phase_of(w2), ft_ref, xe, 8, T)
    forward_level(lambda s: load_pairs(xe, s), phase_of(w3), ft_ref, xd, 1, 8 * T)

    def put_targets(b, carry):
        lanes = pl.ds(pl.multiple_of(b * 128, 128), 128)
        parts = [[[], []], [[], []]]
        for h in range(2):
            a = b * 2 + h
            hc, hs = high_phase(a)
            for k in range(8):
                lc, ls = load_rows(el, slice(k * 8, k * 8 + 8))
                y = load_rows(xd.at[0], pl.ds(k * T + a, 8, stride=8 * T))
                y = turn(turn(y, lc, ls, -1), hc, hs, -1)
                for c in range(2):
                    for t in range(2):
                        parts[c][t].append(y[c][t])

        def write(n, v):
            fo_ref[n : n + v.shape[0], lanes] = v

        put_tiles([[jnp.concatenate(parts[c][t], axis=0) for t in range(2)] for c in range(2)], write)
        return carry

    lax.fori_loop(0, T // 2, put_targets, 0)

    def adjoint_half(p, carry):
        wait_all(1, p)

        def spread(i, carry):
            for r in range(4):
                d = i * 4 + r
                for g, x in enumerate(unpack([recv_a[p, d, n] for n in range(7)])):
                    box = d * (T // 8) + g
                    for c in range(2):
                        for t in range(2):
                            xc[0, c, t, pl.ds((box % 8) * 8 + box // 8, 8, stride=64)] = x[c][t]
            return carry

        lax.fori_loop(0, D // 4, spread, 0)

        def finish(s, t0, tb, out):
            cs, sn = rows_of(p0, p * 64 + s)
            out = turn(out, cs, sn, -1)
            for c in range(2):
                for t in range(2):
                    xa[c, t, pl.ds(pl.multiple_of((p * 64 + s) * 8, 8), 8)] = out[c][t]

        adjoint_level(xc, phase_of(w1, p * 8), at_ref, keep_in(xb), 1, 64)
        adjoint_level(xb, phase_of(w0, p * 64), at_ref, finish, 8, 8)
        return carry

    lax.fori_loop(0, m, adjoint_half, 0)

    def leave(a, carry):
        x = [[jnp.concatenate([xa[c, t, pl.ds(i * 64 + a, 8, stride=8)] for i in range(8 * m)], axis=0) for t in range(2)] for c in range(2)]

        def write(n, v):
            ao_ref[a, n : n + v.shape[0]] = v

        put_tiles(x, write)
        return carry

    lax.fori_loop(0, 8, leave, 0)
    for w in range(2):
        for p in range(m):
            drain_all(w, p)


def one_exchange_shards(forward_weights, adjoint_weights, medium):
    nx, ny = lax.axis_size("sx"), lax.axis_size("sy")
    D, S, R = nx * ny, forward_weights.shape[0], adjoint_weights.shape[0]
    m, T = S // 64, R // 64
    vmem, hbm = pl.BlockSpec(memory_space=pltpu.VMEM), pl.BlockSpec(memory_space=pl.ANY)
    forward_table, adjoint_table = forward_parity_table(), adjoint_parity_table()
    f32 = lambda *shape: pltpu.VMEM(shape, jnp.float32)
    f, b = pl.pallas_call(
        lambda *a: whole_kernel((D, m, T, nx, ny), *a),
        in_specs=[pl.BlockSpec(memory_space=pltpu.SMEM), vmem, hbm, vmem, vmem, hbm],
        out_specs=[vmem, vmem],
        out_shape=[jax.ShapeDtypeStruct((2 * Q, R), jnp.float32), jax.ShapeDtypeStruct((8, 2 * Q, S), jnp.float32)],
        scratch_shapes=[
            f32(2 * Q, R), pltpu.VMEM(adjoint_table.shape, jnp.bfloat16),
            f32(2, 2, S * 8, 128), f32(8, 2, 2, 64, 128), f32(1, 2, 2, 512, 128),
            f32(1, 2, 2, 64 * T, 128), f32(8, 2, 2, 8 * T, 128), f32(2, 2, S * 8, 128),
            f32(2, S, 8, 128), f32(2, S // 8, 8, 128), f32(2, 64, 8, 128), f32(2, 8, 8, 128),
            f32(2, S * 8, 128), f32(2, 2, 64, 128),
            *[f32(m, D, 7, 8, 128) for _ in range(4)],
            pltpu.SemaphoreType.DMA((2, m, D)), pltpu.SemaphoreType.DMA((2, m, D)), pltpu.SemaphoreType.DMA((2,)),
        ],
        compiler_params=pltpu.CompilerParams(
            vmem_limit_bytes=60 * 1024 * 1024, collective_id=0, has_side_effects=True
        ),
    )(medium, forward_weights.transpose(1, 2, 0), adjoint_weights.T, grid_rows(), forward_table, adjoint_table)
    return f.T, b.transpose(0, 2, 1)


def shards(forward_weights, adjoint_weights, medium):
    devices = lax.axis_size("sx") * lax.axis_size("sy")
    S, R = forward_weights.shape[0], adjoint_weights.shape[0]
    one = S == 128 and 2 * devices == 64 and R == 1024 and forward_weights.shape[2] == 2 * Q
    return (one_exchange_shards if one else general_shards)(forward_weights, adjoint_weights, medium)


def solution(mesh):
    in_specs = (P(("sy", "sx"), None, None), P(("sx", "sy"), None), P())
    out_specs = (P(("sx", "sy"), None), P(None, ("sy", "sx"), None))
    return jax.shard_map(shards, mesh=mesh, in_specs=in_specs, out_specs=out_specs, check_vma=False)
```

```python
import math

import jax
import jax.numpy as jnp
import ml_dtypes
import numpy as np
from jax import lax
from jax.experimental import pallas as pl
from jax.experimental.pallas import tpu as pltpu
from jax.sharding import PartitionSpec as P

ORDER = 6
LEVELS = 4
Q = 216
band = 8.0


def cheb_points(n):
    return np.array([(1.0 - math.cos((2 * i + 1) * math.pi / (2 * n))) / 2.0 for i in range(n)])


def child_table(n):
    g = cheb_points(n)
    halves = []
    for bit in range(2):
        m = np.ones((n, n))
        for r in range(n):
            w = (g[r] + bit) / 2.0
            for c in range(n):
                for o in range(n):
                    if o != c:
                        m[r, c] *= (w - g[o]) / (g[c] - g[o])
        halves.append(m)
    return np.stack(
        [np.kron(np.kron(halves[e // 4], halves[e // 2 % 2]), halves[e % 2]) for e in range(8)]
    )


def split_table(table):
    high = table.astype(ml_dtypes.bfloat16)
    low = (table - high.astype(np.float64)).astype(ml_dtypes.bfloat16)
    return jnp.asarray(high), jnp.asarray(low)


def box_coords(index, groups):
    coords = [jnp.zeros_like(index) for _ in range(3)]
    for group in range(groups):
        digit = index // 8 ** (groups - 1 - group) % 8
        bits = (digit // 4, digit // 2 % 2, digit % 2)
        coords = [c * 2 + b for c, b in zip(coords, bits)]
    return [c.astype(jnp.float32) for c in coords]


def point_slopes(src_off, count, groups, medium):
    side = band / float(2**groups)
    g = cheb_points(ORDER).astype(np.float32)
    grid = (np.repeat(g, ORDER * ORDER), np.tile(np.repeat(g, ORDER), ORDER), np.tile(g, ORDER**2))
    corner = box_coords(src_off + jnp.arange(count, dtype=jnp.int32), groups)
    pts = [side * (c[:, None] + o[None, :]) for c, o in zip(corner, grid)]
    radius = jnp.sqrt(pts[0] * pts[0] + pts[1] * pts[1] + pts[2] * pts[2])
    return [p + medium[d + 1] * radius for d, p in enumerate(pts)], medium[0] * radius


def turn_of(u):
    half = jnp.round(2.0 * u)
    y = (2.0 * math.pi) * (u - 0.5 * half)
    sign = 1.0 - 2.0 * (half - 2.0 * jnp.floor(0.5 * half))
    z = y * y
    s = jnp.float32(-1.0 / math.factorial(11))
    for n in (9, 7, 5, 3, 1):
        s = s * z + (1.0 if n % 4 == 1 else -1.0) / math.factorial(n)
    c = jnp.float32(1.0 / math.factorial(12))
    for n in (10, 8, 6, 4, 2, 0):
        c = c * z + (1.0 if n % 4 == 0 else -1.0) / math.factorial(n)
    return sign * c, sign * (s * y)


def pair_phase(src_off, src_count, src_groups, tgt_off, tgt_count, tgt_groups, medium):
    slopes, base = point_slopes(src_off, src_count, src_groups, medium)
    coords = box_coords(tgt_off + jnp.arange(tgt_count, dtype=jnp.int32), tgt_groups)
    u = base[:, None, :]
    for c, a in zip(coords, slopes):
        u = u + ((c + 0.5) / float(2**tgt_groups))[None, :, None] * a[:, None, :]
    return turn_of(u)


def child_phase(src_off, src_count, level, medium):
    slopes, _ = point_slopes(src_off, src_count, LEVELS - level, medium)
    k = np.arange(8)
    u = 0.0
    for bits, a in zip((k // 4, k // 2 % 2, k % 2), slopes):
        step = ((bits - 0.5) / 2.0 ** (level + 2)).astype(np.float32)
        u = u + step[None, :, None] * a[:, None, :]
    return jnp.stack(turn_of(u), axis=1)


def dot3(x, high, low):
    x_high = x.astype(jnp.bfloat16)
    x_low = (x - x_high.astype(jnp.float32)).astype(jnp.bfloat16)
    dot = lambda a, b: jnp.dot(a, b, preferred_element_type=jnp.float32)
    return dot(x_high, high) + dot(x_high, low) + dot(x_low, high)


def forward_kernel(x_ref, w_ref, high_ref, low_ref, o_ref):
    pb, _, _, tb, q = o_ref.shape[0], 2, 8, o_ref.shape[3], o_ref.shape[4]

    def step(e, acc):
        parts = []
        for p in range(pb):
            re, im = x_ref[p, e, 0], x_ref[p, e, 1]
            w_re, w_im = w_ref[p, e, 0], w_ref[p, e, 1]
            res = [re * w_re[k : k + 1] - im * w_im[k : k + 1] for k in range(8)]
            ims = [re * w_im[k : k + 1] + im * w_re[k : k + 1] for k in range(8)]
            parts += res + ims
        return acc + dot3(jnp.concatenate(parts, axis=0), high_ref[e], low_ref[e])

    acc = lax.fori_loop(0, 8, step, jnp.zeros((pb * 16 * tb, q), jnp.float32))
    o_ref[...] = acc.reshape(o_ref.shape)


def adjoint_kernel(y_ref, w_ref, high_ref, low_ref, o_ref):
    sb, tb, q = y_ref.shape[0], y_ref.shape[3], y_ref.shape[4]
    rows = y_ref[...].reshape(sb * 16 * tb, q)

    def step(e, carry):
        z = dot3(rows, high_ref[e], low_ref[e]).reshape(sb, 2, 8, tb, q)
        for s in range(sb):
            w_re, w_im = w_ref[s, e, 0], w_ref[s, e, 1]
            out_re = jnp.zeros((tb, q), jnp.float32)
            out_im = jnp.zeros((tb, q), jnp.float32)
            for k in range(8):
                re, im = z[s, 0, k], z[s, 1, k]
                c, d = w_re[k : k + 1], w_im[k : k + 1]
                out_re += re * c + im * d
                out_im += im * c - re * d
            o_ref[s, e, 0] = out_re
            o_ref[s, e, 1] = out_im
        return carry

    lax.fori_loop(0, 8, step, 0)


def blocks(count, tgt):
    tb = min(tgt, 32)
    return math.gcd(count, max(1, 32 // tb)), tb


def level_call(kernel, operand, phase, tables, out_shape):
    count, tgt, q = operand.shape[0], operand.shape[3], operand.shape[4]
    cb, tb = blocks(count, tgt)
    spec = lambda: pl.BlockSpec((cb, operand.shape[1], operand.shape[2], tb, q), lambda i, j: (i, 0, 0, j, 0))
    return pl.pallas_call(
        kernel,
        grid=(count // cb, tgt // tb),
        in_specs=[
            spec(),
            pl.BlockSpec((cb,) + phase.shape[1:], lambda i, j: (i, 0, 0, 0, 0)),
            pl.BlockSpec(tables[0].shape, lambda i, j: (0, 0, 0)),
            pl.BlockSpec(tables[1].shape, lambda i, j: (0, 0, 0)),
        ],
        out_specs=pl.BlockSpec((cb, out_shape[1], out_shape[2], tb, q), lambda i, j: (i, 0, 0, j, 0)),
        out_shape=jax.ShapeDtypeStruct(out_shape, jnp.float32),
        compiler_params=pltpu.CompilerParams(vmem_limit_bytes=56 * 1024 * 1024),
    )(operand, phase, *tables)


def general_forward_level(x, src_off, level, medium, tables):
    count, _, tgt, q = x.shape
    phase = child_phase(src_off, count, level, medium).reshape(count // 8, 8, 2, 8, q)
    out = level_call(
        forward_kernel, x.reshape(count // 8, 8, 2, tgt, q), phase, tables, (count // 8, 2, 8, tgt, q)
    )
    return out.swapaxes(2, 3).reshape(count // 8, 2, tgt * 8, q)


def general_adjoint_level(y, src_off, level, medium, tables):
    count, _, tgt, q = y.shape
    phase = child_phase(src_off * 8, count * 8, level, medium).reshape(count, 8, 2, 8, q)
    operand = y.reshape(count, 2, tgt // 8, 8, q).swapaxes(2, 3)
    out = level_call(adjoint_kernel, operand, phase, tables, (count, 8, 2, tgt // 8, q))
    return out.reshape(count * 8, 2, tgt // 8, q)


def general_shards(forward_weights, adjoint_weights, medium):
    table = child_table(ORDER) / math.sqrt(8.0)
    forward_tables = split_table(table)
    adjoint_tables = split_table(table.transpose(0, 2, 1))
    sizes = {a: lax.axis_size(a) for a in ("sx", "sy")}
    index = {a: lax.axis_index(a) for a in ("sx", "sy")}
    local_sources = forward_weights.shape[0]
    shots = forward_weights.shape[2] // (2 * Q)
    plan = []
    remaining = ["sx", "sy"]
    width = local_sources
    for _ in range(LEVELS):
        while width < 8:
            axis = remaining.pop(0)
            plan.append(axis)
            width *= sizes[axis]
        plan.append("level")
        width //= 8

    f_in = forward_weights.reshape(local_sources, -1, 2, shots, Q)
    b_in = adjoint_weights.reshape(adjoint_weights.shape[0], 2, shots, Q)
    f_src = (index["sy"] * sizes["sx"] + index["sx"]) * local_sources
    b_tgt = (index["sx"] * sizes["sy"] + index["sy"]) * adjoint_weights.shape[0]
    f_outs, b_outs = [], []
    for shot in range(shots):
        src, tgt, level = f_src, jnp.int32(0), 0
        re, im = f_in[:, :, 0, shot], f_in[:, :, 1, shot]
        c, s = pair_phase(src, re.shape[0], LEVELS, tgt, re.shape[1], 1, medium)
        x = jnp.stack([re * c - im * s, re * s + im * c], axis=1)
        for op in plan:
            if op == "level":
                x = general_forward_level(x, src, level, medium, forward_tables)
                src, tgt, level = src // 8, tgt * 8, level + 1
            else:
                n = sizes[op]
                count, _, width, _ = x.shape
                x = x.reshape(count, 2, n, width // n, Q).transpose(2, 0, 1, 3, 4)
                x = lax.all_to_all(x, op, split_axis=0, concat_axis=0, tiled=True)
                x = x.reshape(n * count, 2, width // n, Q)
                src = src - index[op] * count
                tgt = tgt + index[op] * (width // n)
        c, s = pair_phase(src, x.shape[0], LEVELS - level, tgt, x.shape[2], level + 1, medium)
        re, im = x[:, 0], x[:, 1]
        f_outs.append((re * c + im * s, im * c - re * s))
        src, tgt, level = jnp.int32(0), b_tgt, LEVELS
        re, im = b_in[None, :, 0, shot], b_in[None, :, 1, shot]
        c, s = pair_phase(src, 1, 0, tgt, re.shape[1], LEVELS + 1, medium)
        y = jnp.stack([re * c - im * s, re * s + im * c], axis=1)
        for op in reversed(plan):
            if op == "level":
                y = general_adjoint_level(y, src, level - 1, medium, adjoint_tables)
                src, tgt, level = src * 8, tgt // 8, level - 1
            else:
                n = sizes[op]
                count, _, width, _ = y.shape
                y = y.reshape(n, count // n, 2, width, Q)
                y = lax.all_to_all(y, op, split_axis=0, concat_axis=0, tiled=True)
                y = y.transpose(1, 2, 0, 3, 4).reshape(count // n, 2, n * width, Q)
                src = src + index[op] * (count // n)
                tgt = tgt - index[op] * width
        c, s = pair_phase(src, y.shape[0], LEVELS, tgt, y.shape[2], 1, medium)
        re, im = y[:, 0], y[:, 1]
        b_outs.append((re * c + im * s, im * c - re * s))
    f = jnp.stack([jnp.stack([o[i][0] for o in f_outs], axis=1) for i in range(2)], axis=1)
    b = jnp.stack([jnp.stack([o[i].swapaxes(0, 1) for o in b_outs], axis=2) for i in range(2)], axis=2)
    return f.reshape(f.shape[0], -1), b.reshape(b.shape[0], b.shape[1], -1)


HALF = Q // 2
ROWS = 512


def lane_points():
    t = np.arange(HALF)
    return t, (ORDER - 1 - t // ORDER**2) * ORDER**2 + t % ORDER**2


def parity_tables():
    t, m = lane_points()
    table = child_table(ORDER) / math.sqrt(8.0)
    out = np.zeros((4, 2, 256, 128))
    for e in range(4):
        rows = np.zeros((256, Q))
        rows[:HALF] = table[e][t]
        rows[128 : 128 + HALF] = table[e][m]
        for s, sign in enumerate((1.0, -1.0)):
            out[e, s, :, :HALF] = 0.5 * (rows[:, t] + sign * rows[:, m])
    high = out.astype(ml_dtypes.bfloat16)
    return high, (out - high.astype(np.float64)).astype(ml_dtypes.bfloat16)


def forward_parity_table():
    high, low = parity_tables()
    return jnp.asarray(np.concatenate([high, low], axis=-1))


def adjoint_parity_table():
    parts = [x.swapaxes(-1, -2) for x in parity_tables()]
    return jnp.asarray(np.stack(parts, axis=2))


def split(x):
    high = x.astype(jnp.bfloat16)
    return high, (x - high.astype(jnp.float32)).astype(jnp.bfloat16)


def dot(a, b):
    return jnp.dot(a, b, preferred_element_type=jnp.float32)


def forward_block(load, phase, table_ref, store, pb, kps, tgt):
    total = [None, None]
    for ep in range(4):
        parts = ([], [])
        for p in range(pb):
            a, b = load(p, ep), load(p, ep + 4)
            for kp in kps:
                (ca, sa), (cb, sb) = phase(p, ep, kp), phase(p, ep + 4, kp)
                for c, wa, wb in ((0, ca, cb), (1, sa, sb), (0, sa, sb), (1, ca, cb)):
                    va = [a[c][t] * wa[t] for t in range(2)]
                    vb = [b[c][t] * wb[t] for t in range(2)]
                    parts[0].append(jnp.concatenate([va[0] + vb[1], va[1] + vb[0]], axis=1))
                    parts[1].append(jnp.concatenate([va[0] - vb[1], va[1] - vb[0]], axis=1))
        for s in range(2):
            high, low = split(jnp.concatenate(parts[s], axis=0))
            table = table_ref[ep, s]
            r = dot(high, table) + dot(low, table)
            total[s] = r if total[s] is None else total[s] + r
    even, odd = (x[:, :128] + x[:, 128:] for x in total)
    n = 0
    for p in range(pb):
        for kp in kps:
            q = []
            for _ in range(4):
                rows = slice(n, n + tgt)
                q.append((even[rows] + odd[rows], even[rows] - odd[rows]))
                n += tgt
            for t in range(2):
                rc, si, rs, ci = (x[t] for x in q)
                store(p, kp, t, (rc - si, rs + ci))
                store(p, 7 - kp, t, (rc + si, ci - rs))


def phase_of(w_ref, first=0):
    def phase(s, kp):
        return [[w_ref[t, first + s, i : i + 1] for t in range(2)] for i in (kp, 4 + kp)]

    return phase


def forward_level(load, phase, table_ref, y_ref, parents, tgt):
    pb, kb = min(parents, max(1, ROWS // (16 * tgt))), min(4, max(1, ROWS // (4 * tgt)))
    for g in range(0, 4, kb):

        def body(i, carry):
            def store(p, k, t, values):
                for c in range(2):
                    y_ref[i * pb + p, c, t, k * tgt : (k + 1) * tgt] = values[c]

            source = lambda p, e: (i * pb + p) * 8 + e
            forward_block(
                lambda p, e: load(source(p, e)),
                lambda p, e, kp: phase(source(p, e), kp),
                table_ref, store, pb, range(g, g + kb), tgt,
            )
            return carry

        lax.fori_loop(0, parents // pb, body, 0)


def adjoint_block(load, phase, table_ref, store, pb, tgt):
    parts = ([], [])
    for p in range(pb):
        for kp in range(4):
            a, b = load(p, kp), load(p, 7 - kp)
            for c, sign in ((0, 1), (1, -1), (0, -1), (1, 1)):
                x = [a[c][t] + b[c][t] if sign > 0 else a[c][t] - b[c][t] for t in range(2)]
                parts[0].append(x[0] + x[1])
                parts[1].append(x[0] - x[1])
    rows = [jnp.concatenate(split(jnp.concatenate(x, axis=0)), axis=1) for x in parts]
    for ep in range(4):
        even, odd = (dot(rows[s], table_ref[ep, s, 0]) + dot(rows[s], table_ref[ep, s, 1]) for s in range(2))
        tiles = [slice(0, 128), slice(128, 256)]
        near = [even[:, t] + odd[:, t] for t in tiles]
        far = [even[:, t] - odd[:, t] for t in reversed(tiles)]
        for e, z in ((ep, near), (ep + 4, far)):
            n = 0
            for p in range(pb):
                out = [[None, None], [None, None]]
                for kp in range(4):
                    cs, sn = phase(p, e, kp)
                    for t in range(2):
                        q = [z[t][n + i * tgt : n + (i + 1) * tgt] for i in range(4)]
                        re, im = q[0] * cs[t] + q[1] * sn[t], q[3] * cs[t] - q[2] * sn[t]
                        out[0][t] = re if kp == 0 else out[0][t] + re
                        out[1][t] = im if kp == 0 else out[1][t] + im
                    n += 4 * tgt
                store(p, e, out)


def adjoint_level(y_ref, phase, table_ref, store, parents, tgt):
    tb = min(tgt, 32)
    pb, nt = min(parents, 32 // tb), tgt // tb

    def body(i, carry):
        p0, t0 = (i // nt) * pb, pl.multiple_of((i % nt) * tb, 8)

        def load(p, k):
            rows = pl.ds(pl.multiple_of(k * tgt + t0, 8), tb)
            return [[y_ref[p0 + p, c, t, rows] for t in range(2)] for c in range(2)]

        source = lambda p, e: (p0 + p) * 8 + e
        adjoint_block(
            load,
            lambda p, e, kp: phase(source(p, e), kp),
            table_ref,
            lambda p, e, out: store(source(p, e), t0, tb, out),
            pb, tb,
        )
        return carry

    lax.fori_loop(0, (parents // pb) * nt, body, 0)


def turn(x, c, s, sign=1):
    if sign > 0:
        return [[x[0][t] * c[t] - x[1][t] * s[t] for t in range(2)], [x[0][t] * s[t] + x[1][t] * c[t] for t in range(2)]]
    return [[x[0][t] * c[t] + x[1][t] * s[t] for t in range(2)], [x[1][t] * c[t] - x[0][t] * s[t] for t in range(2)]]


def pack(groups):
    out, rest = [], []
    for x in groups:
        last = x[1][1]
        for i, y in enumerate((x[0][0], x[0][1], x[1][0])):
            out.append(jnp.concatenate([y[:, :HALF], last[:, 20 * i : 20 * i + 20]], axis=1))
        rest.append(last[:, 60:HALF])
    out.append(jnp.concatenate([rest[0], rest[0][:, :16], rest[1], rest[1][:, :16]], axis=1))
    return out


def unpack(x):
    groups = []
    for g in range(2):
        y = x[3 * g : 3 * g + 3]
        tail = x[6][:, 64 * g : 64 * g + 48]
        last = jnp.concatenate([v[:, HALF:] for v in y] + [tail, tail[:, :20]], axis=1)
        groups.append([[y[0], y[1]], [y[2], last]])
    return groups


def join_rows(groups):
    return [[jnp.concatenate([g[c][t] for g in groups], axis=0) for t in range(2)] for c in range(2)]


def grid_rows():
    t, m = lane_points()
    g = cheb_points(ORDER).astype(np.float32)
    full = (np.repeat(g, ORDER * ORDER), np.tile(np.repeat(g, ORDER), ORDER), np.tile(g, ORDER**2))
    out = np.zeros((8, 128), np.float32)
    for d in range(3):
        out[2 * d, :HALF], out[2 * d + 1, :HALF] = full[d][t], full[d][m]
    return jnp.asarray(out)


def bits_of(index, groups):
    coords = [jnp.zeros_like(index) for _ in range(3)]
    for group in range(groups):
        digit = (index >> (3 * (groups - 1 - group))) & 7
        coords = [c * 2 + ((digit >> b) & 1) for c, b in zip(coords, (2, 1, 0))]
    return [c.astype(jnp.float32) for c in coords]


def slopes_of(index, groups, t, grid_ref, med):
    side = band / float(2**groups)
    pts = [side * (c + grid_ref[2 * d + t : 2 * d + t + 1]) for d, c in enumerate(bits_of(index, groups))]
    radius = jnp.sqrt(pts[0] * pts[0] + pts[1] * pts[1] + pts[2] * pts[2])
    return [p + med[d + 1] * radius for d, p in enumerate(pts)], med[0] * radius


def rows_index():
    return lax.broadcasted_iota(jnp.int32, (8, 128), 0)


def fill_level(w_ref, flat_ref, first, count, level, grid_ref, med, p0_ref=None, at=0):
    def body(j, carry):
        i = at + j
        index = first + i * 8 + rows_index()
        for t in range(2):
            slopes, base = slopes_of(index, LEVELS - level, t, grid_ref, med)
            if p0_ref is not None:
                bc, bs = turn_of(base + 0.5 * (slopes[0] + slopes[1] + slopes[2]))
            for kp in range(4):
                u = 0.0
                for bit, a in zip((kp // 4, kp // 2 % 2, kp % 2), slopes):
                    u = u + ((bit - 0.5) / 2.0 ** (level + 2)) * a
                c, s = turn_of(u)
                flat_ref[t, pl.ds(i * 64 + kp, 8, stride=8)] = c
                flat_ref[t, pl.ds(i * 64 + 4 + kp, 8, stride=8)] = s
                if p0_ref is not None:
                    c2, s2 = c * c - s * s, 2.0 * c * s
                    cc, ss, cs, sc = bc * c2, bs * s2, bc * s2, bs * c2
                    for k, v, w in ((kp, cc - ss, cs + sc), (7 - kp, cc + ss, sc - cs)):
                        p0_ref[0, t, pl.ds(i * 64 + k, 8, stride=8)] = v
                        p0_ref[1, t, pl.ds(i * 64 + k, 8, stride=8)] = w
        for t in range(2):
            for n in range(8):
                w_ref[t, i * 8 + n] = flat_ref[t, pl.ds(pl.multiple_of(i * 64 + n * 8, 8), 8)]
        return carry

    lax.fori_loop(0, count // 8, body, 0)


def take_tiles(read):
    out = []
    for n in (0, Q):
        far = [read(n + a, n + a + 36) for a in (180, 144, 108)] + [read(n, n + 20)]
        out.append([read(n, n + 128).T, jnp.concatenate(far, axis=0).T])
    return out


def put_tiles(x, write):
    for c, n in ((0, 0), (1, Q)):
        near, far = x[c][0].T, x[c][1].T
        write(n, near[:HALF])
        for i, a in enumerate((72, 36, 0)):
            write(n + HALF + 36 * i, far[a : a + 36])


def load_pairs(ref, *index):
    return [[ref[(*index, c, t)] for t in range(2)] for c in range(2)]


def load_rows(ref, rows):
    return [[ref[c, t, rows] for t in range(2)] for c in range(2)]


def whole_kernel(
    geo, med, fw_hbm, aw_hbm, grid_ref, ft_hbm, at_hbm, fo_hbm, ao_hbm,
    fw_ref, aw_ref, ft_ref, at_ref, fo_ref, ao_ref, xa, xb, xc, xd, xe, p0, w0, w1, w2, w3, flat, el, send_f, send_a, recv_f, recv_a,
    send_sem, recv_sem, load_sem,
):
    D, m, T, nx, ny = geo
    ix, iy = lax.axis_index("sx"), lax.axis_index("sy")
    me_s, me_t = iy * nx + ix, ix * ny + iy
    med = [med[i] for i in range(4)]
    mesh_id = pl.DeviceIdType.MESH
    at_target = lambda d: (d // ny, lax.rem(d, ny))
    at_source = lambda d: (lax.rem(d, nx), d // nx)
    barrier = pltpu.get_barrier_semaphore()

    def greet(r, carry):
        pl.semaphore_signal(barrier, inc=1, device_id=at_target(lax.rem(me_t + r, D)), device_id_type=mesh_id)
        return carry

    lax.fori_loop(1, D, greet, 0)
    first_loads = [pltpu.make_async_copy(fw_hbm, fw_ref, load_sem.at[0]), pltpu.make_async_copy(ft_hbm, ft_ref, load_sem.at[1])]
    loads = [pltpu.make_async_copy(aw_hbm, aw_ref, load_sem.at[2])]
    for h in range(2):
        loads.append(pltpu.make_async_copy(at_hbm, at_ref.at[:, :, :, pl.ds(128 * h, 128)], load_sem.at[3 + h]))
    for copy in first_loads + loads:
        copy.start()

    mine = (me_t, me_s)
    slot = (me_s, me_t)
    send, recv = (send_f, send_a), (recv_f, recv_a)
    place = (at_target, at_source)

    def block_copy(w, p, d, q):
        return pltpu.make_async_remote_copy(
            src_ref=send[w].at[p, d], dst_ref=recv[w].at[p, q],
            send_sem=send_sem.at[w, p, d], recv_sem=recv_sem.at[w, p, q],
            device_id=place[w](d), device_id_type=mesh_id,
        )

    def over_others(first, step):
        def body(r, carry):
            step(lax.rem(first + r, D))
            return carry

        lax.fori_loop(1, D, body, 0)

    def keep_own(w, p):
        for n in range(7):
            recv[w][p, slot[w], n] = send[w][p, mine[w], n]

    def start_all(w, p):
        over_others(mine[w], lambda d: block_copy(w, p, d, slot[w]).start())
        keep_own(w, p)

    def wait_all(w, p):
        over_others(slot[w], lambda q: block_copy(w, p, q, q).wait_recv())

    def drain_all(w, p):
        over_others(mine[w], lambda d: block_copy(w, p, d, slot[w]).wait_send())

    src = me_s * (64 * m)

    def fill_half(p):
        fill_level(w0, flat, src, 64, 0, grid_ref, med, p0, p * 8)
        fill_level(w1, flat, src // 8, 8, 1, grid_ref, med, None, p)

    fill_half(0)
    for copy in first_loads:
        copy.wait()

    def bring(a, carry):
        x = take_tiles(lambda i, j: fw_ref[a, i:j])
        for c in range(2):
            for t in range(2):
                for i in range(8 * m):
                    xa[c, t, pl.ds(i * 64 + a, 8, stride=8)] = x[c][t][i * 8 : i * 8 + 8]
        return carry

    lax.fori_loop(0, 8, bring, 0)
    pl.semaphore_wait(barrier, D - 1)

    def rows_of(ref, s):
        return load_rows(ref, pl.ds(pl.multiple_of(s * 8, 8), 8))

    per = T // 8
    groups_of = 8 // per
    span = groups_of // 2

    def forward_half(p, carry):
        def load(s):
            cs, sn = rows_of(p0, p * 64 + s)
            return turn(rows_of(xa, p * 64 + s), cs, sn)

        @pl.when(p > 0)
        def _():
            fill_half(p)

        forward_level(load, phase_of(w0, p * 64), ft_ref, xb, 8, 8)

        def forward_part(r, carry):
            rows = pl.ds(pl.multiple_of(r * 32, 32), 32)
            forward_level(lambda s: load_rows(xb.at[s], rows), phase_of(w1, p * 8), ft_ref, xc, 1, 32)

            def fill(a, carry):
                for n in range(span):
                    d = a * groups_of + r * span + n
                    groups = []
                    for g in range(per):
                        groups.append(load_rows(xc.at[0], pl.ds((n * per + g) * 8 + a, 8, stride=32)))
                    for i, v in enumerate(pack(groups)):
                        send_f[p, d, i] = v
                return carry

            lax.fori_loop(0, 8, fill, 0)

            def go(j, carry):
                a = lax.rem(me_t // groups_of + j, 8)
                for n in range(span):
                    d = a * groups_of + r * span + n

                    @pl.when(d != me_t)
                    def _():
                        block_copy(0, p, d, me_s).start()

                return carry

            lax.fori_loop(0, 8, go, 0)
            return carry

        lax.fori_loop(0, 2, forward_part, 0)
        keep_own(0, p)
        return carry

    lax.fori_loop(0, m, forward_half, 0)

    fill_level(w2, flat, 0, 64, 2, grid_ref, med)
    fill_level(w3, flat, 0, 8, 3, grid_ref, med)
    zero = jnp.zeros((8, 128), jnp.int32)

    def low(k, carry):
        for t in range(2):
            v = 0.0
            for c, a in zip(bits_of(k * 8 + rows_index(), 2), slopes_of(zero, 0, t, grid_ref, med)[0]):
                v = v + ((c - 1.5) / 2.0 ** (LEVELS + 1)) * a
            cs, sn = turn_of(v)
            rows = pl.ds(pl.multiple_of(k * 8, 8), 8)
            el[0, t, rows] = cs
            el[1, t, rows] = sn
        return carry

    lax.fori_loop(0, 8, low, 0)

    def high_phase(a):
        out = ([], [])
        for t in range(2):
            slopes, u = slopes_of(zero, 0, t, grid_ref, med)
            for c, s in zip(bits_of(zero + (me_t * T + a), LEVELS - 1), slopes):
                u = u + ((c + 0.5) / 2.0 ** (LEVELS - 1)) * s
            cs, sn = turn_of(u)
            out[0].append(cs)
            out[1].append(sn)
        return out

    for copy in loads:
        copy.wait()

    def take_targets(b, carry):
        lanes = pl.ds(pl.multiple_of(b * 128, 128), 128)
        x = take_tiles(lambda i, j: aw_ref[i:j, lanes])
        for h in range(2):
            a = b * 2 + h
            hc, hs = high_phase(a)
            for k in range(8):
                rows = slice(h * 64 + k * 8, h * 64 + k * 8 + 8)
                lc, ls = load_rows(el, slice(k * 8, k * 8 + 8))
                y = turn(turn([[x[c][t][rows] for t in range(2)] for c in range(2)], lc, ls), hc, hs)
                for c in range(2):
                    for t in range(2):
                        xd[0, c, t, pl.ds(k * T + a, 8, stride=8 * T)] = y[c][t]
        return carry

    lax.fori_loop(0, T // 2, take_targets, 0)

    def keep_in(ref):
        def store(s, t0, tb, out):
            for c in range(2):
                for t in range(2):
                    ref[s, c, t, pl.ds(t0, tb)] = out[c][t]

        return store

    def fill_back(s, t0, tb, out):
        groups = [[[out[c][t][g * 8 : g * 8 + 8] for t in range(2)] for c in range(2)] for g in range(T // 8)]
        for n, v in enumerate(pack(groups)):
            send_a[lax.rem(s, m), s // m, n] = v

    adjoint_level(xd, phase_of(w3), at_ref, keep_in(xe), 1, 8 * T)
    adjoint_level(xe, phase_of(w2), at_ref, fill_back, 8, T)
    for p in range(m):
        start_all(1, p)

    for p in range(m):
        wait_all(0, p)

    def arrived(s):
        return join_rows(unpack([recv_f[lax.rem(s, m), s // m, n] for n in range(7)]))

    forward_level(arrived, phase_of(w2), ft_ref, xe, 8, T)
    forward_level(lambda s: load_pairs(xe, s), phase_of(w3), ft_ref, xd, 1, 8 * T)

    def put_targets(b, carry):
        lanes = pl.ds(pl.multiple_of(b * 128, 128), 128)
        parts = [[[], []], [[], []]]
        for h in range(2):
            a = b * 2 + h
            hc, hs = high_phase(a)
            for k in range(8):
                lc, ls = load_rows(el, slice(k * 8, k * 8 + 8))
                y = load_rows(xd.at[0], pl.ds(k * T + a, 8, stride=8 * T))
                y = turn(turn(y, lc, ls, -1), hc, hs, -1)
                for c in range(2):
                    for t in range(2):
                        parts[c][t].append(y[c][t])

        def write(n, v):
            fo_ref[n : n + v.shape[0], lanes] = v

        put_tiles([[jnp.concatenate(parts[c][t], axis=0) for t in range(2)] for c in range(2)], write)
        return carry

    lax.fori_loop(0, T // 2, put_targets, 0)
    leaving = [pltpu.make_async_copy(fo_ref, fo_hbm, load_sem.at[0])]
    leaving[0].start()

    def adjoint_half(p, carry):
        wait_all(1, p)

        def spread(i, carry):
            for r in range(4):
                d = i * 4 + r
                for g, x in enumerate(unpack([recv_a[p, d, n] for n in range(7)])):
                    box = d * (T // 8) + g
                    for c in range(2):
                        for t in range(2):
                            xc[0, c, t, pl.ds((box % 8) * 8 + box // 8, 8, stride=64)] = x[c][t]
            return carry

        lax.fori_loop(0, D // 4, spread, 0)

        def finish(s, t0, tb, out):
            cs, sn = rows_of(p0, p * 64 + s)
            out = turn(out, cs, sn, -1)
            for c in range(2):
                for t in range(2):
                    xa[c, t, pl.ds(pl.multiple_of((p * 64 + s) * 8, 8), 8)] = out[c][t]

        adjoint_level(xc, phase_of(w1, p * 8), at_ref, keep_in(xb), 1, 64)
        adjoint_level(xb, phase_of(w0, p * 64), at_ref, finish, 8, 8)
        for q in range(m):
            pl.when(p == q)(lambda: leave(q))
        return carry

    def leave(p):
        def body(a, carry):
            x = [
                [jnp.concatenate([xa[c, t, pl.ds((p * 8 + i) * 64 + a, 8, stride=8)] for i in range(8)], axis=0) for t in range(2)]
                for c in range(2)
            ]

            def write(n, v):
                ao_ref[a, n : n + v.shape[0], p * 64 : p * 64 + 64] = v

            put_tiles(x, write)
            if p == m - 1:
                pltpu.make_async_copy(ao_ref.at[a], ao_hbm.at[a], load_sem.at[1 + a]).start()
            return carry

        lax.fori_loop(0, 8, body, 0)

    lax.fori_loop(0, m, adjoint_half, 0)
    for a in range(8):
        leaving.append(pltpu.make_async_copy(ao_ref.at[a], ao_hbm.at[a], load_sem.at[1 + a]))
    for copy in leaving:
        copy.wait()
    for w in range(2):
        for p in range(m):
            drain_all(w, p)


def one_exchange_shards(forward_weights, adjoint_weights, medium):
    nx, ny = lax.axis_size("sx"), lax.axis_size("sy")
    D, S, R = nx * ny, forward_weights.shape[0], adjoint_weights.shape[0]
    m, T = S // 64, R // 64
    vmem, hbm = pl.BlockSpec(memory_space=pltpu.VMEM), pl.BlockSpec(memory_space=pl.ANY)
    forward_table, adjoint_table = forward_parity_table(), adjoint_parity_table()
    f32 = lambda *shape: pltpu.VMEM(shape, jnp.float32)
    f, b = pl.pallas_call(
        lambda *a: whole_kernel((D, m, T, nx, ny), *a),
        in_specs=[pl.BlockSpec(memory_space=pltpu.SMEM), hbm, hbm, vmem, hbm, hbm],
        out_specs=[hbm, hbm],
        out_shape=[jax.ShapeDtypeStruct((2 * Q, R), jnp.float32), jax.ShapeDtypeStruct((8, 2 * Q, S), jnp.float32)],
        scratch_shapes=[
            f32(8, 2 * Q, S), f32(2 * Q, R), pltpu.VMEM(forward_table.shape, jnp.bfloat16),
            pltpu.VMEM((4, 2, 2, 256, 256), jnp.bfloat16), f32(2 * Q, R), f32(8, 2 * Q, S),
            f32(2, 2, S * 8, 128), f32(8, 2, 2, 64, 128), f32(1, 2, 2, 512, 128),
            f32(1, 2, 2, 64 * T, 128), f32(8, 2, 2, 8 * T, 128), f32(2, 2, S * 8, 128),
            f32(2, S, 8, 128), f32(2, S // 8, 8, 128), f32(2, 64, 8, 128), f32(2, 8, 8, 128),
            f32(2, S * 8, 128), f32(2, 2, 64, 128),
            *[f32(m, D, 7, 8, 128) for _ in range(4)],
            pltpu.SemaphoreType.DMA((2, m, D)), pltpu.SemaphoreType.DMA((2, m, D)), pltpu.SemaphoreType.DMA((9,)),
        ],
        compiler_params=pltpu.CompilerParams(
            vmem_limit_bytes=60 * 1024 * 1024, collective_id=0, has_side_effects=True
        ),
    )(medium, forward_weights.transpose(1, 2, 0), adjoint_weights.T, grid_rows(), forward_table, adjoint_table)
    return f.T, b.transpose(0, 2, 1)


def shards(forward_weights, adjoint_weights, medium):
    devices = lax.axis_size("sx") * lax.axis_size("sy")
    S, R = forward_weights.shape[0], adjoint_weights.shape[0]
    one = S == 128 and 2 * devices == 64 and R == 1024 and forward_weights.shape[2] == 2 * Q
    return (one_exchange_shards if one else general_shards)(forward_weights, adjoint_weights, medium)


def solution(mesh):
    in_specs = (P(("sy", "sx"), None, None), P(("sx", "sy"), None), P())
    out_specs = (P(("sx", "sy"), None), P(None, ("sy", "sx"), None))
    return jax.shard_map(shards, mesh=mesh, in_specs=in_specs, out_specs=out_specs, check_vma=False)
```
